32 devices in a mesh: dp: 4 (over y, core), expert: 4 (over z), tensor: 2 (over x).
Axes of the slice: x: 2, y: 2, z: 4, core: 2. Of those that a mesh axis runs over, the one named last changes fastest.
Arguments:
- router_input: bfloat16 [1024, 2048], P(('dp', 'expert'), 'tensor'), may hold values from -6 to 6
- router_weight: bfloat16 [2048, 8], replicated, may hold values from -0.125 to 0.125
- expert_ids: int32 [1024, 2], P(('dp', 'expert', 'tensor')), may hold values from 0 to 7, all different within a row; in each aligned block of 32 rows (0 to 31, 32 to 63, ...) at most 9 rows name the same one
- down_weight: bfloat16 [61440, 2048], P(('expert', 'tensor')), may hold values from -0.0625 to 0.0625
- hidden: bfloat16 [4, 72, 61440], P('dp', None, ('expert', 'tensor')), may hold values from -6 to 6
- grad_output: bfloat16 [1024, 2048], P(('dp', 'expert', 'tensor')), may hold values from -4 to 4
Outputs:
- weight_grad: bfloat16 [61440, 2048], P(('expert', 'tensor', 'dp'))
- hidden_grad: bfloat16 [4, 72, 61440], P('dp', None, ('expert', 'tensor'))
- router_grad: float32 [2048, 8], replicated
- input_grad: bfloat16 [1024, 2048], P(('dp', 'expert', 'tensor'))
The draws below stay inside these ranges and needn't reach their ends.
Inputs may be any that keep to these rules, and one draw needn't show every extreme that they name: `expert_ids`: each row names 2 different experts. Within the 32 rows of one device no expert is named more than 9 times, and some device's rows name some expert exactly 9 times.
All inputs are finite; a program needn't handle non-finite values.
Results may differ from the reference program's by a relative error of at most 0.018.
Values may be sent and summed in bfloat16 or wider, within the bound.
A program may use at most 192 MiB of HBM per device.

```python
import math
import jax
import jax.numpy as jnp
import numpy as np
from jax import lax

D = 2048
FF = 7680
EXPERTS = 8
TOPK = 2
TOK_DEV = 32
CAP = 9
SOURCES = 8
TOKENS = 1024
N_DP = 4


def shard_levels(key, shape, split, smallest, largest):
    level, own = 1.0, jax.random.fold_in(key, 6)
    for axis_at, blocks in split:
        draws = jnp.exp(jax.random.uniform(jax.random.fold_in(own, axis_at), (blocks,), jnp.float32, smallest / len(split), largest / len(split)))
        level = level * jnp.repeat(draws, shape[axis_at] // blocks).reshape([-1 if axis == axis_at else 1 for axis in range(len(shape))])
    return level


def deal_out(key, own, number, rows, amount, top, most, slope):
    order = jax.random.permutation(key, amount)
    crowded, common = shares(amount, rows * top, most, slope, True), shares(amount, rows * top, most, slope, False)
    places = jnp.arange(amount)

    def named(tallies, offset_by):
        used = int((tallies > 0).sum())
        fixed = max(1, used // 4)
        shifted = fixed + (places - fixed + offset_by * (used - fixed)) % max(1, amount - fixed)
        return jnp.zeros((amount,), jnp.int32).at[order[jnp.where(places < fixed, places, shifted)]].set(jnp.asarray(tallies, jnp.int32))

    tallies = jnp.where(number % 4 == 0, named(crowded, number // 4), named(common, number - number // 4 - 1))
    mixed = jax.random.permutation(jax.random.fold_in(own, 3), amount)
    donor, receiver = mixed[0:amount // 2 * 2:2], mixed[1:amount // 2 * 2:2]
    slack = jnp.minimum(tallies[donor] - 1, most - tallies[receiver]) // 2
    slack = jnp.where((donor == order[0]) | (receiver == order[0]) | (tallies[receiver] == 0), 0, jnp.maximum(slack, 0))
    shifted = jax.random.randint(jax.random.fold_in(own, 4), (amount // 2,), 0, 1 << 20) % (slack + 1)
    tallies = tallies.at[donor].add(-shifted).at[receiver].add(shifted)
    items = jnp.searchsorted(jnp.cumsum(tallies), jnp.arange(rows * top), side="right").astype(jnp.int32)
    listing = items.reshape(top, rows).T
    listing = listing[jax.random.permutation(jax.random.fold_in(own, 1), rows)]
    offset_by = jax.random.randint(jax.random.fold_in(own, 2), (rows, 1), 0, top)
    return jnp.take_along_axis(listing, (jnp.arange(top)[None, :] + offset_by) % top, axis=1)


def shares(count, total, bound, slope, full):
    weights = [(1 << 20) // math.isqrt(grade ** slope) + 1 for grade in range(1, count + 1)]
    largest = bound if full else min(bound, max(-(-total // count), total * weights[0] // sum(weights)))
    least = 1 if total - largest >= count - 1 else 0
    given, spare = [largest] + [least] * (count - 1), total - largest - least * (count - 1)
    while spare > 0:
        movable = [i for i in range(1, count) if given[i] < largest] or [i for i in range(1, count) if given[i] < bound]
        mass, left = sum([weights[i] for i in movable]), spare
        for i in movable:
            extra = min(bound - given[i], max(1, left * weights[i] // mass), spare)
            given[i] = given[i] + extra
            spare = spare - extra
    return np.array(given)


def centred(stream_key, dims, spread, bound, cuts=(), kind=jnp.bfloat16):
    drawn = jax.random.normal(stream_key, dims, jnp.float32) * spread
    if len(cuts) > 0:
        drawn = shard_levels(stream_key, dims, cuts, -0.22, 0.18) * drawn
    return jnp.clip(drawn, min=-bound, max=bound).astype(kind)


def setup_inputs(seed: int = 0) -> dict:
    splits = jax.random.split(jax.random.key(seed), 7)
    router_input = centred(splits[0], (TOKENS, D), 1.0, 6.0, ((0, 16), (1, 2)))
    router_weight = centred(splits[1], (D, EXPERTS), D ** -0.5, 0.125)
    expert_ids_keys = jax.random.split(jax.random.fold_in(splits[2], 1), TOKENS // TOK_DEV)
    expert_ids_turns = jax.random.permutation(jax.random.fold_in(splits[2], 3), TOKENS // TOK_DEV)
    expert_ids = jax.vmap(lambda own, number: deal_out(jax.random.fold_in(splits[2], 2), own, number, TOK_DEV, EXPERTS, TOPK, CAP, 2))(expert_ids_keys, expert_ids_turns).reshape((TOKENS, TOPK))
    down_weight = centred(splits[3], (EXPERTS * FF, D), FF ** -0.5, 0.0625, ((0, 8),))
    hidden = centred(splits[4], (N_DP, SOURCES * CAP, EXPERTS * FF), 1.0, 6.0, ((0, 4), (2, 8)))
    grad_output = centred(splits[5], (TOKENS, D), 0.25, 4.0, ((0, 32),))
    return dict(router_input=router_input, router_weight=router_weight, expert_ids=expert_ids, down_weight=down_weight, hidden=hidden, grad_output=grad_output)


def reference(router_input, router_weight, expert_ids, down_weight, hidden, grad_output):
    logits = jnp.dot(router_input, router_weight, preferred_element_type=jnp.float32)
    labels = jnp.arange(EXPERTS, dtype=jnp.int32)
    onehot_int = (expert_ids[:, :, None] == labels).astype(jnp.int32)
    onehot = onehot_int.astype(jnp.float32)
    picked = jnp.sum(onehot * logits[:, None, :], axis=2)
    first_gate = jax.nn.sigmoid(picked[:, 0] - picked[:, 1])
    second_gate = jax.nn.sigmoid(picked[:, 1] - picked[:, 0])
    gate_values = jnp.stack([first_gate, second_gate], axis=1)
    gate_low = gate_values.astype(jnp.bfloat16)
    blocks = TOKENS // TOK_DEV
    flat_hits = onehot_int.reshape(blocks, TOK_DEV * TOPK, EXPERTS)
    before = jnp.cumsum(flat_hits, axis=1) - flat_hits
    slot_pos = jnp.sum(before * flat_hits, axis=2).reshape(blocks, TOK_DEV, TOPK)
    slot_ids = jnp.arange(CAP, dtype=jnp.int32)
    dispatch_table = onehot.reshape(blocks, TOK_DEV, TOPK, EXPERTS, 1) * (slot_pos[:, :, :, None, None] == slot_ids).astype(jnp.float32)
    table_groups = dispatch_table.reshape(N_DP, SOURCES, TOK_DEV, TOPK, EXPERTS, CAP)
    grad_groups = grad_output.reshape(N_DP, SOURCES, TOK_DEV, D)
    gate_groups = gate_low.reshape(N_DP, SOURCES, TOK_DEV, TOPK)
    expert_weights = down_weight.reshape(EXPERTS, FF, D)

    def one_expert(pieces):
        expert_grad, expert_gate, expert_hidden, expert_weight = pieces
        expert_image = jnp.dot(expert_grad, expert_weight.T, preferred_element_type=jnp.float32)
        hidden_part = (expert_gate[:, None] * expert_image).astype(jnp.bfloat16)
        gate_part = jnp.sum(expert_hidden.astype(jnp.float32) * expert_image, axis=1)
        gated = (expert_gate[:, None] * expert_grad.astype(jnp.float32)).astype(jnp.bfloat16)
        weight_term = jnp.dot(expert_hidden.T, gated, preferred_element_type=jnp.float32).astype(jnp.bfloat16)
        return hidden_part, gate_part, weight_term

    def one_group(running_total, pieces):
        table_i, grad_i, gate_i, hidden_i = pieces
        slot_table = jnp.sum(table_i, axis=2)
        packed_grad = jnp.einsum("srec,srd->escd", slot_table, grad_i.astype(jnp.float32))
        packed_grad = packed_grad.astype(jnp.bfloat16).reshape(EXPERTS, SOURCES * CAP, D)
        packed_gate = jnp.einsum("srkec,srk->esc", table_i, gate_i.astype(jnp.float32)).reshape(EXPERTS, SOURCES * CAP)
        hidden_split = hidden_i.reshape(SOURCES * CAP, EXPERTS, FF).transpose(1, 0, 2)
        hidden_part, gate_part, weight_term = lax.map(one_expert, (packed_grad, packed_gate, hidden_split, expert_weights))
        running_total = running_total + weight_term.reshape(EXPERTS * FF, D).astype(jnp.float32)
        token_grad = jnp.einsum("srkec,esc->srk", table_i, gate_part.reshape(EXPERTS, SOURCES, CAP))
        hidden_rows = hidden_part.transpose(1, 0, 2).reshape(SOURCES * CAP, EXPERTS * FF)
        return running_total, (hidden_rows, token_grad)

    zero_total = jnp.zeros((EXPERTS * FF, D), jnp.float32)
    running_total, outputs = lax.scan(one_group, zero_total, (table_groups, grad_groups, gate_groups, hidden))
    hidden_grad, token_grad = outputs
    weight_grad = running_total.astype(jnp.bfloat16)
    gate_grad = token_grad.reshape(TOKENS, TOPK)
    mixed_term = jnp.sum(gate_values * gate_grad, axis=1, keepdims=True)
    logit_part = gate_values * (gate_grad - mixed_term)
    logit_grad = jnp.sum(onehot * logit_part[:, :, None], axis=1)
    input_grad = jnp.dot(logit_grad, router_weight.astype(jnp.float32).T, precision=lax.Precision.HIGHEST).astype(jnp.bfloat16)
    router_grad = jnp.dot(router_input.astype(jnp.float32).T, logit_grad, precision=lax.Precision.HIGHEST)
    return weight_grad, hidden_grad, router_grad, input_grad
```

```python
import functools

import jax
import jax.numpy as jnp
from jax import lax
from jax.experimental import pallas as pl
from jax.experimental.pallas import tpu as pltpu
from jax.sharding import PartitionSpec as P


PAD = 16
LANES = 128
HALF = 8
VMEM_LIMIT = 54 * 1000 * 1000
STORE_LIMIT = 8 * 1000 * 1000
OUT = pltpu.VMEM
EXACT = lax.Precision.HIGHEST
CONTRACT_LAST = (((1,), (1,)), ((), ()))
CONTRACT_FIRST = (((0,), (0,)), ((), ()))


def iota(shape, axis):
    return lax.broadcasted_iota(jnp.int32, shape, axis)


def exchange_kernel(
    groups, expert_ranks, tensor_ranks, capacity, tile,
    ids_hbm, router_weight_hbm, grad_hbm, router_input_ref, down_ref, hidden_ref,
    weight_grad_ref, hidden_out, input_grad_ref, router_grad_ref,
    ids_ref, router_weight_ref, grad_ref, full_input, weights, hidden_rows,
    send_low, recv_low, send_top, recv_top, send_gate, recv_gate, send_back, recv_back,
    send_sum, recv_sum, packed, pulled, hidden_near, gated_near, hidden_far, gated_far,
    load_sem, weight_sem, hidden_sem, own_sem,
    input_send, input_recv, low_send, low_recv, top_send, top_recv, gate_send, gate_recv,
    hidden_send, hidden_recv, gated_send, gated_recv, back_send, back_recv,
    sum_send, sum_recv, whole_send, whole_recv,
):
    f32, bf16 = jnp.float32, jnp.bfloat16
    group = lax.axis_index("dp")
    expert = lax.axis_index("expert")
    tensor = lax.axis_index("tensor")
    sources = expert_ranks * tensor_ranks
    source = expert * tensor_ranks + tensor
    devices = groups * sources
    me = group * sources + source
    slots, width = hidden_ref.shape
    part = width // groups
    experts = router_weight_ref.shape[0]
    tokens = grad_ref.shape[0]
    span = router_input_ref.shape[1]
    rows = sources * PAD
    tiles = width // tile

    def remote(src, dst, send, recv, device):
        return pltpu.make_async_remote_copy(
            src_ref=src, dst_ref=dst, send_sem=send, recv_sem=recv,
            device_id=device, device_id_type=pl.DeviceIdType.MESH,
        )

    def drain(ref, sem):
        pltpu.make_async_copy(ref, ref, sem).wait()

    def weight_copy(i):
        return pltpu.make_async_copy(
            down_ref.at[pl.ds(i * tile, tile)], weights.at[pl.ds(i * tile, tile)],
            weight_sem.at[i],
        )

    dps = [(group + d) % groups for d in range(groups)]
    ers = [(expert + e) % expert_ranks for e in range(expert_ranks)]
    trs = [(tensor + t) % tensor_ranks for t in range(tensor_ranks)]
    peers = [
        (ers[e] * tensor_ranks + trs[t], {"dp": group, "expert": ers[e], "tensor": trs[t]})
        for e in range(expert_ranks) for t in range(tensor_ranks) if e or t
    ]
    others = [
        (
            (dps[d] * expert_ranks + ers[e]) * tensor_ranks + trs[t],
            {"dp": dps[d], "expert": ers[e], "tensor": trs[t]},
        )
        for e in range(expert_ranks) for d in range(groups) for t in range(tensor_ranks)
        if e or d or t
    ]

    barrier = pltpu.get_barrier_semaphore()
    for _, where in others:
        pl.semaphore_signal(
            barrier, inc=1, device_id=where, device_id_type=pl.DeviceIdType.MESH
        )

    loads = [
        pltpu.make_async_copy(ids_hbm, ids_ref, load_sem.at[0]),
        pltpu.make_async_copy(grad_hbm, grad_ref, load_sem.at[1]),
        pltpu.make_async_copy(router_weight_hbm, router_weight_ref, load_sem.at[2]),
        pltpu.make_async_copy(
            router_input_ref.at[pl.ds(pl.multiple_of(tensor * tokens, tokens), tokens)],
            full_input.at[tensor], load_sem.at[3],
        ),
    ]
    for copy in loads:
        copy.start()

    hidden_load = pltpu.make_async_copy(hidden_ref, hidden_rows, hidden_sem)
    hidden_load.start()

    @pl.loop(0, tiles)
    def _(i):
        weight_copy(i).start()

    own_hidden = pltpu.make_async_copy(
        hidden_ref.at[:, pl.ds(pl.multiple_of(group * part, LANES), part)],
        hidden_near.at[0, pl.ds(0, slots)], own_sem,
    )
    own_hidden.start()

    tail = hidden_near.shape[1] - slots
    for buffer in (hidden_near, hidden_far, gated_near, gated_far):
        buffer[:, slots:, :] = jnp.zeros((2, tail, buffer.shape[2]), bf16)
    loads[0].wait()
    labels = iota((experts, tokens), 0)
    pick_first = (ids_ref[0:1, :] == labels).astype(f32)
    pick_second = (ids_ref[1:2, :] == labels).astype(f32)
    pick_both = pick_first + pick_second
    same = (iota((tokens, tokens), 0) == iota((tokens, tokens), 1)).astype(f32)
    first = lax.dot_general(same, pick_first, CONTRACT_LAST, preferred_element_type=f32)
    second = lax.dot_general(same, pick_second, CONTRACT_LAST, preferred_element_type=f32)
    earlier = (iota((tokens, tokens), 1) < iota((tokens, tokens), 0)).astype(f32)
    before = lax.dot_general(pick_both, earlier, CONTRACT_LAST, preferred_element_type=f32)
    spread_rows = ((iota((rows, experts), 0) >> 4) == iota((rows, experts), 1)).astype(f32)
    hit = jnp.dot(spread_rows, pick_both, preferred_element_type=f32)
    rank = jnp.dot(spread_rows, before, preferred_element_type=f32)
    slot = (iota((rows, tokens), 0) & (PAD - 1)).astype(f32)
    table = jnp.where((hit > 0.5) & (jnp.abs(rank - slot) < 0.5), 1.0, 0.0).astype(f32)
    low_table = table.reshape(sources, PAD, tokens)[:, :HALF].reshape(sources * HALF, tokens)
    top_table = jnp.where((pick_both > 0.5) & (jnp.abs(before - HALF) < 0.5), 1.0, 0.0)
    loads[1].wait()
    send_low[...] = (
        jnp.dot(low_table.astype(bf16), grad_ref[...], preferred_element_type=f32)
        .astype(bf16)
        .reshape(send_low.shape)
    )
    send_top[...] = jnp.dot(
        top_table.astype(bf16), grad_ref[...], preferred_element_type=f32
    ).reshape(send_top.shape)

    pl.semaphore_wait(barrier, devices - 1)

    for t in range(1, tensor_ranks):
        remote(
            router_input_ref.at[pl.ds(pl.multiple_of(trs[t] * tokens, tokens), tokens)],
            full_input.at[tensor], input_send, input_recv, {"tensor": trs[t]},
        ).start()
    for to, where in peers:
        remote(send_low.at[to], recv_low.at[source], low_send, low_recv, where).start()
        remote(send_top.at[to], recv_top.at[source], top_send, top_recv, where).start()

    core = group % 2
    half = group // 2
    beside = half * 2 + (1 - core)
    across = (1 - half) * 2 + core
    diagonal = (1 - half) * 2 + (1 - core)
    hidden_to = (
        (beside, hidden_near.at[1, pl.ds(0, slots)], 0),
        (across, hidden_far.at[0, pl.ds(0, slots)], 1),
        (diagonal, hidden_far.at[1, pl.ds(0, slots)], 2),
    )
    hidden_copies = [
        remote(
            hidden_ref.at[:, pl.ds(pl.multiple_of(to * part, LANES), part)], landing,
            hidden_send.at[k], hidden_recv.at[k], {"dp": to},
        )
        for to, landing, k in hidden_to
    ]
    for copy in hidden_copies:
        copy.start()

    recv_top[pl.ds(source, 1)] = send_top[pl.ds(source, 1)]
    recv_low[pl.ds(source, 1)] = send_low[pl.ds(source, 1)]

    height = packed.shape[0]
    column = iota((height, sources * HALF), 1)
    pick_low = (
        iota((height, sources * HALF), 0) == capacity * (column >> 3) + (column & (HALF - 1))
    ).astype(bf16)
    slot_row = iota((height, sources), 0)
    slot_base = capacity * iota((height, sources), 1)
    pick_top = (slot_row == slot_base + HALF).astype(bf16)
    pick_source = ((slot_row >= slot_base) & (slot_row < slot_base + capacity)).astype(f32)
    slot_at = iota((height, LANES), 0) - capacity * jnp.sum(
        pick_source * iota((height, sources), 1).astype(f32), axis=1, keepdims=True
    ).astype(jnp.int32)
    slot_lane = (slot_at == iota((height, LANES), 1)) & (iota((height, LANES), 0) < slots)

    def pull(begin, end):
        for i in range(begin, end):
            weight_copy(i).wait()
        at = slice(begin * tile, end * tile)
        term = jnp.dot(hidden_rows[:, at], weights[at, :], preferred_element_type=f32)
        pulled[...] = pulled[...] + term if begin else term

    cuts = chunk_bounds(tiles)
    early = [c for c in cuts if c[1] <= tiles // 2]
    hidden_load.wait()
    for begin, end in early:
        pull(begin, end)

    loads[2].wait()
    loads[3].wait()
    drain(full_input.at[pl.ds(0, tensor_ranks - 1)], input_recv)
    logits = jnp.zeros((tokens, experts), f32)
    for h in range(tensor_ranks):
        logits = logits + lax.dot_general(
            full_input[h], router_weight_ref[:, h * span : (h + 1) * span], CONTRACT_LAST,
            preferred_element_type=f32,
        )
    chosen = jnp.sum(first * logits, axis=1, keepdims=True)
    rival = jnp.sum(second * logits, axis=1, keepdims=True)
    first_gate = jax.nn.sigmoid(chosen - rival)
    second_gate = jax.nn.sigmoid(rival - chosen)
    gates = first * first_gate + second * second_gate
    low = gates.astype(bf16).astype(f32)
    gate_rows = lax.dot_general(spread_rows, low, CONTRACT_LAST, preferred_element_type=f32)
    slot_gate = jnp.sum(table * gate_rows, axis=1, keepdims=True)
    row_lane = (iota((rows, LANES), 0) & (PAD - 1)) == iota((rows, LANES), 1)
    send_gate[...] = lax.dot_general(
        spread_rows, jnp.where(row_lane, slot_gate, 0.0), CONTRACT_FIRST,
        preferred_element_type=f32,
    ).reshape(send_gate.shape)
    for to, where in peers:
        remote(send_gate.at[to], recv_gate.at[source], gate_send, gate_recv, where).start()
    recv_gate[pl.ds(source, 1)] = send_gate[pl.ds(source, 1)]

    for begin, end in cuts[len(early) :]:
        pull(begin, end)

    drain(recv_low.at[pl.ds(0, sources - 1)], low_recv)
    drain(recv_top.at[pl.ds(0, sources - 1)], top_recv)
    model = packed.shape[1]
    packed[...] = (
        jnp.dot(
            pick_low, recv_low[...].reshape(sources * HALF, model), preferred_element_type=f32
        )
        + jnp.dot(
            pick_top, recv_top[...].reshape(sources, model).astype(bf16),
            preferred_element_type=f32,
        )
    ).astype(bf16)
    partial = jnp.sum(packed[:slots].astype(f32) * pulled[...], axis=1, keepdims=True)
    send_back[...] = lax.dot_general(
        pick_source[:slots], jnp.where(slot_lane[:slots], partial, 0.0), CONTRACT_FIRST,
        precision=EXACT, preferred_element_type=f32,
    ).reshape(send_back.shape)
    for to, where in peers:
        remote(send_back.at[to], recv_back.at[source], back_send, back_recv, where).start()
    recv_back[pl.ds(source, 1)] = send_back[pl.ds(source, 1)]

    drain(recv_gate.at[pl.ds(0, sources - 1)], gate_recv)
    gate_lanes = jnp.dot(
        pick_source, recv_gate[...].reshape(sources, LANES), preferred_element_type=f32
    )
    gate_column = jnp.sum(jnp.where(slot_lane, gate_lanes, 0.0), axis=1, keepdims=True)[:slots]
    gated_near[0, :slots] = (gate_column * packed[:slots].astype(f32)).astype(bf16)

    mine = gated_near.at[0, pl.ds(0, slots)]
    from_beside = gated_near.at[1, pl.ds(0, slots)]
    from_across = gated_far.at[0, pl.ds(0, slots)]
    from_diagonal = gated_far.at[1, pl.ds(0, slots)]
    to_across = remote(mine, from_across, gated_send.at[0], gated_recv.at[0], {"dp": across})
    to_across.start()
    to_beside = remote(mine, from_beside, gated_send.at[1], gated_recv.at[1], {"dp": beside})
    to_beside.start()
    relay = remote(
        from_across, from_diagonal, gated_send.at[2], gated_recv.at[2], {"dp": beside}
    )

    def image_tile(i):
        at = slice(i * tile, (i + 1) * tile)
        image = lax.dot_general(
            weights[at, :], packed[...], CONTRACT_LAST, preferred_element_type=f32
        ).T[:slots]
        hidden_out[:, at] = (gate_column * image).astype(bf16)

    for i in range(tiles // 2):
        image_tile(i)

    drain(recv_back.at[pl.ds(0, sources - 1)], back_recv)
    back_rows = jnp.dot(
        spread_rows, recv_back[...].reshape(sources, LANES), precision=EXACT,
        preferred_element_type=f32,
    )
    returned = jnp.sum(jnp.where(row_lane, back_rows, 0.0), axis=1, keepdims=True)
    gate_grad = lax.dot_general(
        table * returned, spread_rows, CONTRACT_FIRST, precision=EXACT, preferred_element_type=f32
    )
    mixed = jnp.sum(gates * gate_grad, axis=1, keepdims=True)
    logit_grad = gates * (gate_grad - mixed)
    chunk = experts // groups
    block = (span * tensor_ranks) // sources
    terms = split_terms(logit_grad)
    for h in range(tensor_ranks):
        local = lax.dot_general(
            terms, full_input[h], CONTRACT_FIRST, preferred_element_type=f32
        )
        local = local[:experts] + local[experts : 2 * experts] + local[2 * experts :]
        for b in range(span // block):
            x = h * (span // block) + b
            for d in range(groups):
                send_sum[d * sources + x] = local[
                    d * chunk : (d + 1) * chunk, b * block : (b + 1) * block
                ]
    for to, where in others:
        remote(send_sum.at[to], recv_sum.at[me], sum_send, sum_recv, where).start()
    recv_sum[pl.ds(me, 1)] = send_sum[pl.ds(me, 1)]
    input_grad_ref[...] = jnp.dot(
        logit_grad, router_weight_ref[...].astype(f32), precision=EXACT,
        preferred_element_type=f32,
    ).astype(bf16)

    for i in range(tiles // 2, tiles):
        image_tile(i)

    depth = 2 * height
    step = part_tile(part)

    def weight_rows(hidden_pair, gated_pair, i):
        at = slice(i * step, (i + 1) * step)
        return at, lax.dot_general(
            hidden_pair[:, :, at].reshape(depth, step),
            gated_pair[...].reshape(depth, model),
            CONTRACT_FIRST, preferred_element_type=f32,
        )

    own_hidden.wait()
    hidden_copies[0].wait_recv()
    to_beside.wait_recv()
    for i in range(part // step):
        at, term = weight_rows(hidden_near, gated_near, i)
        weight_grad_ref[at, :] = term.astype(bf16)

    to_across.wait_recv()
    relay.start()
    drain(recv_sum.at[pl.ds(0, devices - 1)], sum_recv)
    router_grad_ref[pl.ds(me, 1)] = jnp.sum(recv_sum[...], axis=0, keepdims=True)
    for to, where in others:
        remote(
            router_grad_ref.at[me], router_grad_ref.at[me], whole_send, whole_recv, where
        ).start()

    for copy in hidden_copies[1:]:
        copy.wait_recv()
    relay.wait_recv()
    for i in range(part // step):
        at, term = weight_rows(hidden_far, gated_far, i)
        weight_grad_ref[at, :] = (weight_grad_ref[at, :].astype(f32) + term).astype(bf16)

    for copy in (*hidden_copies, to_across, to_beside, relay):
        copy.wait_send()
    drain(send_low.at[pl.ds(0, sources - 1)], low_send)
    drain(send_top.at[pl.ds(0, sources - 1)], top_send)
    drain(full_input.at[pl.ds(0, tensor_ranks - 1)], input_send)
    drain(send_gate.at[pl.ds(0, sources - 1)], gate_send)
    drain(send_back.at[pl.ds(0, sources - 1)], back_send)
    drain(send_sum.at[pl.ds(0, devices - 1)], sum_send)
    drain(router_grad_ref.at[pl.ds(0, devices - 1)], whole_recv)
    drain(router_grad_ref.at[pl.ds(0, devices - 1)], whole_send)


def split_terms(value):
    parts = []
    for _ in range(3):
        part = value.astype(jnp.bfloat16).astype(jnp.float32)
        parts.append(part)
        value = value - part
    return jnp.concatenate(parts, axis=1).astype(jnp.bfloat16)


def chunk_bounds(tiles):
    bounds, at = [], 0
    while at < tiles:
        size = 3 if tiles - at > 3 else max(1, (tiles - at) // 2 + (tiles - at) % 2)
        bounds.append((at, at + size))
        at += size
    return bounds


def store_kernel(
    sources, weight_ref, hidden_ref, input_ref, router_ref,
    weight_out, hidden_out, input_out, router_out, router_rows, store_sem,
):
    cuts = store_sem.shape[0] - 3
    rows = weight_ref.shape[0] // cuts
    stores = [
        pltpu.make_async_copy(
            weight_ref.at[pl.ds(c * rows, rows)], weight_out.at[pl.ds(c * rows, rows)],
            store_sem.at[c],
        )
        for c in range(cuts)
    ]
    stores.append(pltpu.make_async_copy(hidden_ref, hidden_out, store_sem.at[cuts]))
    stores.append(pltpu.make_async_copy(input_ref, input_out, store_sem.at[cuts + 1]))
    for store in stores:
        store.start()
    pieces, chunk, block = router_ref.shape
    for piece in range(pieces):
        d, x = piece // sources, piece % sources
        router_rows[d * chunk : (d + 1) * chunk, x * block : (x + 1) * block] = router_ref[piece]
    stores.append(pltpu.make_async_copy(router_rows, router_out, store_sem.at[cuts + 2]))
    stores[-1].start()
    for store in stores:
        store.wait()


def by_kernels(router_input, router_weight, expert_ids, down_weight, hidden, grad_output):
    f32, bf16 = jnp.float32, jnp.bfloat16
    tokens, model = grad_output.shape
    experts = router_weight.shape[1]
    groups = lax.axis_size("dp")
    expert_ranks = lax.axis_size("expert")
    tensor_ranks = lax.axis_size("tensor")
    sources = expert_ranks * tensor_ranks
    devices = groups * sources
    slots, width = hidden.shape[1:]
    height = -(-slots // LANES) * LANES
    tile = tile_of(width)
    span = router_input.shape[1]
    part = width // groups
    vmem = pl.BlockSpec(memory_space=pltpu.VMEM)
    hbm = pl.BlockSpec(memory_space=pl.ANY)
    dma = pltpu.SemaphoreType.DMA
    piece = (devices, experts // groups, model // sources)
    weight_grad, hidden_grad, input_grad, router_parts = pl.pallas_call(
        functools.partial(
            exchange_kernel, groups, expert_ranks, tensor_ranks, slots // sources, tile
        ),
        out_shape=(
            OUT((part, model), bf16),
            OUT((slots, width), bf16),
            OUT((tokens, model), bf16),
            OUT(piece, f32),
        ),
        in_specs=[hbm] * 6,
        out_specs=(vmem,) * 4,
        scratch_shapes=[
            pltpu.VMEM((2, tokens), jnp.int32),
            pltpu.VMEM((experts, model), bf16),
            pltpu.VMEM((tokens, model), bf16),
            pltpu.VMEM((tensor_ranks, tokens, span), bf16),
            pltpu.VMEM((width, model), bf16),
            pltpu.VMEM((slots, width), bf16),
            pltpu.VMEM((sources, HALF, model), bf16),
            pltpu.VMEM((sources, HALF, model), bf16),
            pltpu.VMEM((sources, 1, model), f32),
            pltpu.VMEM((sources, 1, model), f32),
            pltpu.VMEM((sources, 1, LANES), f32),
            pltpu.VMEM((sources, 1, LANES), f32),
            pltpu.VMEM((sources, 1, LANES), f32),
            pltpu.VMEM((sources, 1, LANES), f32),
            pltpu.VMEM(piece, f32),
            pltpu.VMEM(piece, f32),
            pltpu.VMEM((height, model), bf16),
            pltpu.VMEM((slots, model), f32),
            pltpu.VMEM((2, height, part), bf16),
            pltpu.VMEM((2, height, model), bf16),
            pltpu.VMEM((2, height, part), bf16),
            pltpu.VMEM((2, height, model), bf16),
            dma((4,)), dma((width // tile,)), dma, dma,
            dma, dma, dma, dma, dma, dma, dma, dma,
            dma((3,)), dma((3,)), dma((3,)), dma((3,)), dma, dma,
            dma, dma, dma, dma,
        ],
        compiler_params=pltpu.CompilerParams(
            collective_id=0, has_side_effects=True, vmem_limit_bytes=VMEM_LIMIT
        ),
        name="exchange",
    )(expert_ids.T, router_weight.T, grad_output, router_input, down_weight, hidden[0])
    weight_grad, hidden_grad, input_grad, router_grad = pl.pallas_call(
        functools.partial(store_kernel, sources),
        out_shape=(
            jax.ShapeDtypeStruct((part, model), bf16),
            jax.ShapeDtypeStruct((slots, width), bf16),
            jax.ShapeDtypeStruct((tokens, model), bf16),
            jax.ShapeDtypeStruct((experts, model), f32),
        ),
        in_specs=[vmem] * 4,
        out_specs=(hbm,) * 4,
        scratch_shapes=[pltpu.VMEM((experts, model), f32), dma((part // part_tile(part) + 3,))],
        compiler_params=pltpu.CompilerParams(vmem_limit_bytes=STORE_LIMIT),
        name="store",
    )(weight_grad, hidden_grad, input_grad, router_parts)
    return weight_grad, hidden_grad[None], router_grad.T, input_grad


def part_tile(part):
    return 384 if part % 384 == 0 else LANES


def tile_of(width):
    for tile in (512, 384, 256):
        if width % tile == 0:
            return tile
    return LANES


def kernels_fit(router_input, router_weight, expert_ids, down_weight, hidden, grad_output):
    groups = lax.axis_size("dp")
    sources = lax.axis_size("expert") * lax.axis_size("tensor")
    slots, width = hidden.shape[1:]
    tokens, model = grad_output.shape
    experts = router_weight.shape[1]
    return (
        groups == 4
        and sources == experts
        and experts % groups == 0
        and slots % 8 == 0
        and slots // sources == HALF + 1
        and slots <= LANES
        and tokens % 16 == 0
        and width % (groups * LANES) == 0
        and model % (sources * LANES) == 0
        and 2 * (width * model + 4 * slots * width + 8 * slots * model) < 48 * 1000 * 1000
    )


def per_device(*arrays):
    return by_kernels(*arrays) if kernels_fit(*arrays) else by_collectives(*arrays)


def by_collectives(router_input, router_weight, expert_ids, down_weight, hidden, grad_output):
    token_rows = grad_output.shape[0]
    model_width = grad_output.shape[1]
    expert_count = router_weight.shape[1]
    choose_count = expert_ids.shape[1]
    expert_ranks = lax.axis_size("expert")
    tensor_ranks = lax.axis_size("tensor")
    sources = expert_ranks * tensor_ranks
    spread = sources // expert_count
    capacity = hidden.shape[1] // sources
    full_input = lax.all_to_all(router_input, "tensor", split_axis=0, concat_axis=1, tiled=True)
    logits = jnp.dot(full_input, router_weight, preferred_element_type=jnp.float32)
    labels = jnp.arange(expert_count, dtype=jnp.int32)
    onehot_int = (expert_ids[:, :, None] == labels).astype(jnp.int32)
    onehot = onehot_int.astype(jnp.float32)
    picked = jnp.sum(onehot * logits[:, None, :], axis=2)
    first_gate = jax.nn.sigmoid(picked[:, 0] - picked[:, 1])
    second_gate = jax.nn.sigmoid(picked[:, 1] - picked[:, 0])
    gate_values = jnp.stack([first_gate, second_gate], axis=1)
    gate_low = gate_values.astype(jnp.bfloat16)
    flat_hits = onehot_int.reshape(token_rows * choose_count, expert_count)
    before = jnp.cumsum(flat_hits, axis=0) - flat_hits
    slot_pos = jnp.sum(before * flat_hits, axis=1).reshape(token_rows, choose_count)
    slot_ids = jnp.arange(capacity, dtype=jnp.int32)
    dispatch_table = onehot[:, :, :, None] * (slot_pos[:, :, None, None] == slot_ids).astype(
        jnp.float32
    )
    slot_table = jnp.sum(dispatch_table, axis=1).astype(jnp.bfloat16)
    packed_grad = jnp.einsum(
        "rec,rd->ecd", slot_table, grad_output, preferred_element_type=jnp.float32
    ).astype(jnp.bfloat16)
    packed_gate = jnp.einsum("rkec,rk->ec", dispatch_table, gate_low.astype(jnp.float32)).astype(
        jnp.bfloat16
    )
    send_grad = jnp.repeat(packed_grad, spread, axis=0)
    send_gate = jnp.repeat(packed_gate, spread, axis=0)
    recv_grad, recv_gate = (
        lax.all_to_all(send_grad, ("expert", "tensor"), split_axis=0, concat_axis=0, tiled=True),
        lax.all_to_all(send_gate, ("expert", "tensor"), split_axis=0, concat_axis=0, tiled=True),
    )
    recv_grad = recv_grad.reshape(sources * capacity, model_width)
    recv_gate = recv_gate.reshape(sources * capacity).astype(jnp.float32)
    hidden_rows = hidden[0]
    gated_grad = (recv_gate[:, None] * recv_grad.astype(jnp.float32)).astype(jnp.bfloat16)
    expert_image = lax.dot_general(
        recv_grad, down_weight, (((1,), (1,)), ((), ())), preferred_element_type=jnp.float32
    )
    hidden_part = (recv_gate[:, None] * expert_image).astype(jnp.bfloat16)
    gate_partial = jnp.sum(hidden_rows.astype(jnp.float32) * expert_image, axis=1).reshape(
        sources, capacity
    )
    returned = lax.all_to_all(
        gate_partial, ("expert", "tensor"), split_axis=0, concat_axis=0, tiled=True
    )
    expert_sums = jnp.sum(returned.reshape(expert_count, spread, capacity), axis=1)
    gate_grad = jnp.einsum("rkec,ec->rk", dispatch_table, expert_sums)
    mixed_term = jnp.sum(gate_values * gate_grad, axis=1, keepdims=True)
    logit_part = gate_values * (gate_grad - mixed_term)
    logit_grad = jnp.sum(onehot * logit_part[:, :, None], axis=1)
    input_grad = jnp.dot(
        logit_grad, router_weight.astype(jnp.float32).T, precision=lax.Precision.HIGHEST
    ).astype(jnp.bfloat16)
    router_local = jnp.dot(
        full_input.astype(jnp.float32).T, logit_grad, precision=lax.Precision.HIGHEST
    )
    router_grad = lax.psum(router_local, ("dp", "expert", "tensor"))
    hidden_all = lax.all_to_all(hidden_rows, "dp", split_axis=1, concat_axis=0, tiled=True)
    gated_all = lax.all_gather(gated_grad, "dp", axis=0, tiled=True)
    weight_sum = lax.dot_general(
        hidden_all, gated_all, (((0,), (0,)), ((), ())), preferred_element_type=jnp.float32
    ).astype(jnp.bfloat16)
    return (weight_sum, hidden_part[None], router_grad, input_grad)


def solution(mesh):
    return jax.shard_map(
        per_device,
        mesh=mesh,
        in_specs=(
            P(("dp", "expert"), "tensor"),
            P(),
            P(("dp", "expert", "tensor"), None),
            P(("expert", "tensor"), None),
            P("dp", None, ("expert", "tensor")),
            P(("dp", "expert", "tensor"), None),
        ),
        out_specs=(
            P(("expert", "tensor", "dp"), None),
            P("dp", None, ("expert", "tensor")),
            P(),
            P(("dp", "expert", "tensor"), None),
        ),
        check_vma=False,
    )
```

```python
import functools

import jax
import jax.numpy as jnp
from jax import lax
from jax.experimental import pallas as pl
from jax.experimental.pallas import tpu as pltpu
from jax.sharding import PartitionSpec as P


PAD = 16
LANES = 128
HALF = 8
VMEM_LIMIT = 50 * 1000 * 1000
WEIGHT_LIMIT = 24 * 1000 * 1000
OUT = pltpu.VMEM
PAUSE = 8
LAST_TILES = 2
EXACT = lax.Precision.HIGHEST
CONTRACT_LAST = (((1,), (1,)), ((), ()))
CONTRACT_FIRST = (((0,), (0,)), ((), ()))


def iota(shape, axis):
    return lax.broadcasted_iota(jnp.int32, shape, axis)


def exchange_kernel(
    groups, expert_ranks, tensor_ranks, capacity, tile,
    ids_hbm, router_weight_hbm, grad_hbm, router_input_ref, down_ref, hidden_ref,
    near_ref, hidden_near, gated_near, hidden_far, gated_far, hidden_out, input_grad_ref,
    router_grad_ref, ids_ref, router_weight_ref, grad_ref, own_input, weights, hidden_rows,
    send_low, recv_low, send_top, recv_top, send_back, recv_back,
    send_info, recv_info, column_input, slot_weight, slot_sign, logit_rows, group_sums,
    send_logit, recv_logit, packed, pulled,
    load_sem, weight_sem, hidden_sem, own_sem,
    logit_send, logit_recv, low_send, low_recv, top_send, top_recv,
    hidden_send, hidden_recv, gated_send, gated_recv, back_send, back_recv,
    info_send, info_recv, column_send, column_recv, sum_send, sum_recv, whole_send, whole_recv,
):
    f32, bf16 = jnp.float32, jnp.bfloat16
    group = lax.axis_index("dp")
    expert = lax.axis_index("expert")
    tensor = lax.axis_index("tensor")
    sources = expert_ranks * tensor_ranks
    source = expert * tensor_ranks + tensor
    slots, width = hidden_ref.shape
    part = width // groups
    experts = router_weight_ref.shape[0]
    tokens = grad_ref.shape[0]
    span = router_input_ref.shape[1]
    feats = span // expert_ranks
    rows = sources * PAD
    tiles = width // tile

    def remote(src, dst, send, recv, device):
        return pltpu.make_async_remote_copy(
            src_ref=src, dst_ref=dst, send_sem=send, recv_sem=recv,
            device_id=device, device_id_type=pl.DeviceIdType.MESH,
        )

    def drain(ref, sem):
        pltpu.make_async_copy(ref, ref, sem).wait()

    cuts = chunk_bounds(tiles)
    weight_copies = [
        pltpu.make_async_copy(
            down_ref.at[pl.ds(begin * tile, (end - begin) * tile)],
            weights.at[pl.ds(begin * tile, (end - begin) * tile)], weight_sem.at[c],
        )
        for c, (begin, end) in enumerate(cuts)
    ]

    ers = [(expert + e) % expert_ranks for e in range(expert_ranks)]
    trs = [(tensor + t) % tensor_ranks for t in range(tensor_ranks)]
    peers = [
        (ers[e] * tensor_ranks + trs[t], {"dp": group, "expert": ers[e], "tensor": trs[t]})
        for e in range(expert_ranks) for t in range(tensor_ranks) if e or t
    ]
    core = group % 2
    half = group // 2
    beside = half * 2 + (1 - core)
    across = (1 - half) * 2 + core
    diagonal = (1 - half) * 2 + (1 - core)
    mates = [
        {"dp": to, "expert": expert, "tensor": tensor} for to in (across, diagonal, beside)
    ]

    loads = [
        pltpu.make_async_copy(ids_hbm, ids_ref, load_sem.at[0]),
        pltpu.make_async_copy(grad_hbm, grad_ref, load_sem.at[1]),
        pltpu.make_async_copy(router_weight_hbm, router_weight_ref, load_sem.at[2]),
        pltpu.make_async_copy(router_input_ref, own_input, load_sem.at[3]),
        pltpu.make_async_copy(
            router_input_ref.at[:, pl.ds(pl.multiple_of(expert * feats, LANES), feats)],
            column_input.at[expert], load_sem.at[4],
        ),
    ]
    for copy in loads:
        copy.start()

    hidden_load = pltpu.make_async_copy(hidden_ref, hidden_rows, hidden_sem)
    hidden_load.start()

    for copy in weight_copies:
        copy.start(priority=1)
    own_hidden = pltpu.make_async_copy(
        hidden_ref.at[:, pl.ds(pl.multiple_of(group * part, LANES), part)],
        hidden_near.at[0, pl.ds(0, slots)], own_sem,
    )
    own_hidden.start()

    barrier = pltpu.get_barrier_semaphore()
    for where in [place for _, place in peers] + mates:
        pl.semaphore_signal(
            barrier, inc=1, device_id=where, device_id_type=pl.DeviceIdType.MESH
        )

    send_info[...] = jnp.zeros_like(send_info)
    tail = hidden_near.shape[1] - slots
    for buffer in (hidden_near, hidden_far, gated_near, gated_far):
        buffer[:, slots:, :] = jnp.zeros((2, tail, buffer.shape[2]), bf16)
    loads[0].wait()
    labels = iota((experts, tokens), 0)
    pick_first = (ids_ref[0:1, :] == labels).astype(f32)
    pick_second = (ids_ref[1:2, :] == labels).astype(f32)
    pick_both = pick_first + pick_second
    earlier = (iota((tokens, tokens), 1) < iota((tokens, tokens), 0)).astype(f32)
    before = lax.dot_general(pick_both, earlier, CONTRACT_LAST, preferred_element_type=f32)
    spread_rows = ((iota((rows, experts), 0) >> 4) == iota((rows, experts), 1)).astype(f32)
    hit = jnp.dot(spread_rows, pick_both, preferred_element_type=f32)
    rank = jnp.dot(spread_rows, before, preferred_element_type=f32)
    slot = (iota((rows, tokens), 0) & (PAD - 1)).astype(f32)
    table = jnp.where((hit > 0.5) & (jnp.abs(rank - slot) < 0.5), 1.0, 0.0).astype(f32)
    low_table = table.reshape(sources, PAD, tokens)[:, :HALF].reshape(sources * HALF, tokens)
    top_table = jnp.where((pick_both > 0.5) & (jnp.abs(before - HALF) < 0.5), 1.0, 0.0)
    loads[1].wait()
    wide = send_low.shape[3]
    for h in range(2):
        send_low[h] = (
            jnp.dot(
                low_table.astype(bf16), grad_ref[:, h * wide : (h + 1) * wide],
                preferred_element_type=f32,
            )
            .astype(bf16)
            .reshape(send_low.shape[1:])
        )
    send_top[...] = jnp.dot(
        top_table.astype(bf16), grad_ref[...], preferred_element_type=f32
    ).reshape(send_top.shape)

    loads[2].wait()
    loads[3].wait()
    own_weight = router_weight_ref[:, pl.ds(pl.multiple_of(tensor * span, LANES), span)]

    def part_logits(t):
        return lax.dot_general(
            own_weight, own_input[pl.ds(pl.multiple_of(trs[t] * tokens, tokens), tokens)],
            CONTRACT_LAST, preferred_element_type=f32,
        )

    for t in range(1, tensor_ranks):
        send_logit[t] = part_logits(t)
    send_logit[0] = part_logits(0)

    pl.semaphore_wait(barrier, len(peers) + len(mates))

    for t in range(1, tensor_ranks):
        remote(
            send_logit.at[t], recv_logit.at[t], logit_send, logit_recv, {"tensor": trs[t]}
        ).start()
    for to, where in peers:
        remote(
            send_low.at[0, to], recv_low.at[0, source], low_send, low_recv.at[0], where
        ).start()
    for to, where in peers:
        remote(
            send_low.at[1, to], recv_low.at[1, source], low_send, low_recv.at[1], where
        ).start()
        remote(send_top.at[to], recv_top.at[source], top_send, top_recv, where).start()

    hidden_to = (
        (beside, hidden_near.at[1, pl.ds(0, slots)], 0),
        (across, hidden_far.at[0, pl.ds(0, slots)], 1),
        (diagonal, hidden_far.at[1, pl.ds(0, slots)], 2),
    )
    hidden_copies = [
        remote(
            hidden_rows.at[:, pl.ds(pl.multiple_of(to * part, LANES), part)], landing,
            hidden_send.at[k], hidden_recv.at[k], {"dp": to},
        )
        for to, landing, k in hidden_to
    ]
    hidden_load.wait()
    for copy in hidden_copies:
        copy.start()

    recv_top[pl.ds(source, 1)] = send_top[pl.ds(source, 1)]
    for h in range(2):
        recv_low[h, pl.ds(source, 1)] = send_low[h, pl.ds(source, 1)]

    height = packed.shape[0]
    column = iota((height, sources * HALF), 1)
    pick_low = (
        iota((height, sources * HALF), 0) == capacity * (column >> 3) + (column & (HALF - 1))
    ).astype(bf16)
    slot_row = iota((height, sources), 0)
    slot_base = capacity * iota((height, sources), 1)
    pick_top = (slot_row == slot_base + HALF).astype(bf16)
    pick_source = ((slot_row >= slot_base) & (slot_row < slot_base + capacity)).astype(f32)
    slot_at = iota((height, LANES), 0) - capacity * jnp.sum(
        pick_source * iota((height, sources), 1).astype(f32), axis=1, keepdims=True
    ).astype(jnp.int32)
    slot_lane = (slot_at == iota((height, LANES), 1)) & (iota((height, LANES), 0) < slots)

    def pull(c):
        begin, end = cuts[c]
        weight_copies[c].wait()
        at = slice(begin * tile, end * tile)
        term = jnp.dot(hidden_rows[:, at], weights[at, :], preferred_element_type=f32)
        pulled[...] = pulled[...] + term if c else term

    early = 1
    for c in range(early):
        pull(c)

    drain(recv_logit.at[pl.ds(0, tensor_ranks - 1)], logit_recv)
    logits = send_logit[0]
    for t in range(1, tensor_ranks):
        logits = logits + recv_logit[t]
    chosen = jnp.sum(pick_first * logits, axis=0, keepdims=True)
    rival = jnp.sum(pick_second * logits, axis=0, keepdims=True)
    first_gate = jax.nn.sigmoid(chosen - rival)
    second_gate = jax.nn.sigmoid(rival - chosen)
    numbered = before + PAD * labels.astype(f32)
    send_info[0:1, :tokens] = jnp.sum(pick_first * numbered, axis=0, keepdims=True)
    send_info[1:2, :tokens] = jnp.sum(pick_second * numbered, axis=0, keepdims=True)
    send_info[2:3, :tokens] = first_gate * second_gate
    send_info[3:4, :tokens] = first_gate.astype(bf16).astype(f32)
    send_info[4:5, :tokens] = second_gate.astype(bf16).astype(f32)
    for _, where in peers:
        remote(send_info, recv_info.at[source], info_send, info_recv, where).start()
    recv_info[pl.ds(source, 1)] = send_info[...][None]

    for c in range(early, len(cuts)):
        pull(c)

    drain(recv_info.at[pl.ds(0, sources - 1)], info_recv)
    for h in range(2):
        drain(recv_low.at[h, pl.ds(0, sources - 1)], low_recv.at[h])
    drain(recv_top.at[pl.ds(0, sources - 1)], top_recv)
    model = packed.shape[1]
    for h in range(2):
        at = slice(h * wide, (h + 1) * wide)
        packed[:, at] = (
            jnp.dot(
                pick_low, recv_low[h].reshape(sources * HALF, wide), preferred_element_type=f32
            )
            + jnp.dot(
                pick_top, recv_top[:, :, at].reshape(sources, wide).astype(bf16),
                preferred_element_type=f32,
            )
        ).astype(bf16)
    partial = jnp.sum(packed[:slots].astype(f32) * pulled[...], axis=1, keepdims=True)
    own_lane = (iota((slots, LANES), 1) - PAD * source) == slot_at[:slots]
    send_back[...] = lax.dot_general(
        pick_source[:slots], jnp.where(own_lane, partial, 0.0), CONTRACT_FIRST,
        precision=EXACT, preferred_element_type=f32,
    )
    for _, where in peers:
        remote(send_back, recv_back.at[source], back_send, back_recv, where).start()
    for e in range(1, expert_ranks):
        remote(
            own_input.at[:, pl.ds(pl.multiple_of(ers[e] * feats, LANES), feats)],
            column_input.at[expert], column_send, column_recv, {"expert": ers[e]},
        ).start()
    recv_back[pl.ds(source, 1)] = send_back[...][None]

    known = recv_info[...].reshape(sources * HALF, LANES)
    known = jnp.concatenate([known, jnp.zeros((LANES - sources * HALF, LANES), f32)], axis=0).T
    slot_lanes = iota((tokens, LANES), 1).astype(f32)
    label_lanes = PAD * iota((tokens, experts), 1).astype(f32)
    gate_lanes = jnp.zeros((height, LANES), f32)
    for x in range(sources):
        one, two, share, one_gate, two_gate = (
            known[:tokens, x * HALF + k : x * HALF + k + 1] for k in range(5)
        )
        slot_weight[x] = jnp.where(
            slot_lanes == one, share, jnp.where(slot_lanes == two, -share, 0.0)
        )
        slot_sign[x] = jnp.where(
            (one >= label_lanes) & (one < label_lanes + PAD), 1.0, 0.0
        ) - jnp.where((two >= label_lanes) & (two < label_lanes + PAD), 1.0, 0.0)
        gate_row = jnp.sum(
            jnp.where(
                slot_lanes == one, one_gate, jnp.where(slot_lanes == two, two_gate, 0.0)
            ),
            axis=0, keepdims=True,
        )
        gate_lanes = gate_lanes + pick_source[:, x : x + 1] * gate_row
    gate_column = jnp.sum(
        jnp.where(own_lane, gate_lanes[:slots], 0.0), axis=1, keepdims=True
    )
    gated_near[0, :slots] = (gate_column * packed[:slots].astype(f32)).astype(bf16)

    fold = model * 3 // 8 // LANES * LANES
    spans = (pl.ds(0, fold), pl.ds(fold, model - fold))

    def gated_part(buffer, k, h):
        return buffer.at[k, pl.ds(0, slots), spans[h]]

    to_across, to_beside, relays = [], [], []
    for h in range(2):
        mine = gated_part(gated_near, 0, h)
        from_beside = gated_part(gated_near, 1, h)
        from_across = gated_part(gated_far, 0, h)
        from_diagonal = gated_part(gated_far, 1, h)
        to_across.append(
            remote(mine, from_across, gated_send.at[0, h], gated_recv.at[0, h], {"dp": across})
        )
        to_beside.append(
            remote(mine, from_beside, gated_send.at[1, h], gated_recv.at[1, h], {"dp": beside})
        )
        relays.append(
            remote(
                from_across, from_diagonal, gated_send.at[2, h], gated_recv.at[2, h],
                {"dp": beside},
            )
        )
    to_across[0].start()
    for copy in to_beside:
        copy.start()

    def image_tile(i):
        at = slice(i * tile, (i + 1) * tile)
        image = lax.dot_general(
            weights[at, :], packed[...], CONTRACT_LAST, preferred_element_type=f32
        ).T[:slots]
        hidden_out[:, at] = (gate_column * image).astype(bf16)

    pause = tiles * PAUSE // 15
    for i in range(pause):
        image_tile(i)

    drain(recv_back.at[pl.ds(0, sources - 1)], back_recv)
    returned = recv_back[0]
    for e in range(1, experts):
        returned = returned + recv_back[e]
    for x in range(sources):
        logit_rows[x] = slot_sign[x] * jnp.sum(
            slot_weight[x] * returned[x : x + 1], axis=1, keepdims=True
        )
    terms = split_terms(logit_rows[...].reshape(sources * tokens, experts))
    loads[4].wait()
    drain(column_input.at[pl.ds(0, expert_ranks - 1)], column_recv)
    sums = lax.dot_general(
        terms, column_input[...].reshape(sources * tokens, feats), CONTRACT_FIRST,
        preferred_element_type=f32,
    )
    group_sums[pl.ds(group, 1)] = (
        sums[:experts] + sums[experts : 2 * experts] + sums[2 * experts :]
    )[None]
    for where in mates:
        remote(
            group_sums.at[group], group_sums.at[group], sum_send, sum_recv, where
        ).start()
    to_across[1].start()
    input_grad_ref[...] = jnp.dot(
        logit_rows[pl.ds(source, 1)].reshape(tokens, experts),
        router_weight_ref[...].astype(f32), precision=EXACT,
        preferred_element_type=f32,
    ).astype(bf16)

    later = max(pause, tiles - LAST_TILES)
    for i in range(pause, later):
        image_tile(i)

    to_across[0].wait_recv()
    relays[0].start()
    drain(group_sums.at[pl.ds(0, groups - 1)], sum_recv)
    total = group_sums[0]
    for d in range(1, groups):
        total = total + group_sums[d]
    router_grad_ref[pl.ds(source, 1)] = total[None]
    for _, where in peers:
        remote(
            router_grad_ref.at[source], router_grad_ref.at[source], whole_send, whole_recv, where
        ).start()
    for i in range(later, tiles):
        image_tile(i)


    step = part_tile(part)

    to_across[1].wait_recv()
    relays[1].start()
    own_hidden.wait()
    hidden_copies[0].wait_recv()
    for copy in to_beside:
        copy.wait_recv()
    for i in range(near_ref.shape[0] // step):
        at = slice(i * step, (i + 1) * step)
        near_ref[at, :] = pair_product(hidden_near, gated_near, at).astype(bf16)

    for copy in hidden_copies[1:]:
        copy.wait_recv()
    for copy in relays:
        copy.wait_recv()
    for copy in (*hidden_copies, *to_across, *to_beside, *relays):
        copy.wait_send()
    drain(send_low.at[:, pl.ds(0, sources - 1)], low_send)
    drain(send_top.at[pl.ds(0, sources - 1)], top_send)
    drain(recv_logit.at[pl.ds(0, tensor_ranks - 1)], logit_send)
    drain(recv_back.at[pl.ds(0, sources - 1)], back_send)
    drain(recv_info.at[pl.ds(0, sources - 1)], info_send)
    drain(column_input.at[pl.ds(0, expert_ranks - 1)], column_send)
    drain(group_sums.at[pl.ds(0, groups - 1)], sum_send)
    drain(router_grad_ref.at[pl.ds(0, sources - 1)], whole_recv)
    drain(router_grad_ref.at[pl.ds(0, sources - 1)], whole_send)


def split_terms(value):
    parts = []
    for _ in range(3):
        part = value.astype(jnp.bfloat16).astype(jnp.float32)
        parts.append(part)
        value = value - part
    return jnp.concatenate(parts, axis=1).astype(jnp.bfloat16)


def chunk_bounds(tiles):
    bounds, at = [], 0
    while at < tiles:
        size = 3 if tiles - at > 3 else max(1, (tiles - at) // 2 + (tiles - at) % 2)
        bounds.append((at, at + size))
        at += size
    return bounds


def pair_product(hidden_ref, gated_ref, at):
    depth = hidden_ref.shape[0] * hidden_ref.shape[1]
    return lax.dot_general(
        hidden_ref[:, :, at].reshape(depth, at.stop - at.start),
        gated_ref[...].reshape(depth, gated_ref.shape[2]),
        CONTRACT_FIRST, preferred_element_type=jnp.float32,
    )


def weight_kernel(
    tensor_ranks, near_ref, hidden_near, gated_near, hidden_far, gated_far, hidden_ref, input_ref, router_ref,
    weight_out, hidden_out, input_out, router_out, weight_rows, router_rows, store_sem,
):
    bounds = row_bounds(weight_rows.shape[0])
    ready = near_ref.shape[0]
    cuts = len(bounds)
    stores = [
        pltpu.make_async_copy(hidden_ref, hidden_out, store_sem.at[cuts]),
        pltpu.make_async_copy(input_ref, input_out, store_sem.at[cuts + 1]),
    ]
    for store in stores:
        store.start()
    for c, (begin, end) in enumerate(bounds):
        at = slice(begin, end)
        far = pair_product(hidden_far, gated_far, at)
        if end <= ready:
            near = near_ref[at, :].astype(jnp.float32)
        else:
            near = pair_product(hidden_near, gated_near, at)
        weight_rows[at, :] = (far + near).astype(weight_rows.dtype)
        rows = pl.ds(begin, end - begin)
        stores.append(
            pltpu.make_async_copy(weight_rows.at[rows], weight_out.at[rows], store_sem.at[c])
        )
        stores[-1].start()
    sources, _, feats = router_ref.shape
    for x in range(sources):
        e, t = x // tensor_ranks, x % tensor_ranks
        column = (t * (sources // tensor_ranks) + e) * feats
        router_rows[:, column : column + feats] = router_ref[x]
    stores.append(pltpu.make_async_copy(router_rows, router_out, store_sem.at[cuts + 2]))
    stores[-1].start()
    for store in stores:
        store.wait()


def by_kernels(router_input, router_weight, expert_ids, down_weight, hidden, grad_output):
    f32, bf16 = jnp.float32, jnp.bfloat16
    tokens, model = grad_output.shape
    experts = router_weight.shape[1]
    groups = lax.axis_size("dp")
    expert_ranks = lax.axis_size("expert")
    tensor_ranks = lax.axis_size("tensor")
    sources = expert_ranks * tensor_ranks
    slots, width = hidden.shape[1:]
    height = -(-slots // LANES) * LANES
    tile = tile_of(width)
    span = router_input.shape[1]
    part = width // groups
    vmem = pl.BlockSpec(memory_space=pltpu.VMEM)
    hbm = pl.BlockSpec(memory_space=pl.ANY)
    dma = pltpu.SemaphoreType.DMA
    feats = span // expert_ranks
    near, *pairs, hidden_grad, input_grad, router_parts = pl.pallas_call(
        functools.partial(
            exchange_kernel, groups, expert_ranks, tensor_ranks, slots // sources, tile
        ),
        out_shape=(
            OUT((near_rows(part), model), bf16),
            OUT((2, height, part), bf16),
            OUT((2, height, model), bf16),
            OUT((2, height, part), bf16),
            OUT((2, height, model), bf16),
            OUT((slots, width), bf16),
            OUT((tokens, model), bf16),
            OUT((sources, experts, feats), f32),
        ),
        in_specs=[hbm] * 6,
        out_specs=(vmem,) * 8,
        scratch_shapes=[
            pltpu.VMEM((2, tokens), jnp.int32),
            pltpu.VMEM((experts, model), bf16),
            pltpu.VMEM((tokens, model), bf16),
            pltpu.VMEM((tensor_ranks * tokens, span), bf16),
            pltpu.VMEM((width, model), bf16),
            pltpu.VMEM((slots, width), bf16),
            pltpu.VMEM((2, sources, HALF, model // 2), bf16),
            pltpu.VMEM((2, sources, HALF, model // 2), bf16),
            pltpu.VMEM((sources, 1, model), f32),
            pltpu.VMEM((sources, 1, model), f32),
            pltpu.VMEM((sources, LANES), f32),
            pltpu.VMEM((experts, sources, LANES), f32),
            pltpu.VMEM((HALF, LANES), f32),
            pltpu.VMEM((sources, HALF, LANES), f32),
            pltpu.VMEM((expert_ranks, tensor_ranks * tokens, feats), bf16),
            pltpu.VMEM((sources, tokens, LANES), f32),
            pltpu.VMEM((sources, tokens, experts), f32),
            pltpu.VMEM((sources, tokens, experts), f32),
            pltpu.VMEM((groups, experts, feats), f32),
            pltpu.VMEM((tensor_ranks, experts, tokens), f32),
            pltpu.VMEM((tensor_ranks, experts, tokens), f32),
            pltpu.VMEM((height, model), bf16),
            pltpu.VMEM((slots, model), f32),
            dma((5,)), dma((len(chunk_bounds(width // tile)),)), dma, dma,
            dma, dma, dma, dma((2,)), dma, dma,
            dma((3,)), dma((3,)), dma((3, 2)), dma((3, 2)), dma, dma,
            dma, dma, dma, dma, dma, dma, dma, dma,
        ],
        compiler_params=pltpu.CompilerParams(
            collective_id=0, has_side_effects=True, vmem_limit_bytes=VMEM_LIMIT
        ),
        name="exchange",
    )(expert_ids.T, router_weight.T, grad_output, router_input, down_weight, hidden[0])
    weight_grad, hidden_grad, input_grad, router_grad = pl.pallas_call(
        functools.partial(weight_kernel, tensor_ranks),
        out_shape=(
            jax.ShapeDtypeStruct((part, model), bf16),
            jax.ShapeDtypeStruct((slots, width), bf16),
            jax.ShapeDtypeStruct((tokens, model), bf16),
            jax.ShapeDtypeStruct((experts, model), f32),
        ),
        in_specs=[vmem] * 8,
        out_specs=(hbm,) * 4,
        scratch_shapes=[
            pltpu.VMEM((part, model), bf16),
            pltpu.VMEM((experts, model), f32),
            dma((len(row_bounds(part)) + 3,)),
        ],
        compiler_params=pltpu.CompilerParams(vmem_limit_bytes=WEIGHT_LIMIT),
        name="weight_grad",
    )(near, *pairs, hidden_grad, input_grad, router_parts)
    return weight_grad, hidden_grad[None], router_grad.T, input_grad


def near_rows(part):
    step = part_tile(part)
    return part // step * 3 // 5 * step


def row_bounds(part):
    units, ready, bounds, at = part // LANES, near_rows(part) // LANES, [], 0
    while at < units:
        stop = ready if at < ready else units
        size = min(stop - at, 2 if at == 0 or at >= ready else 3)
        bounds.append((at * LANES, (at + size) * LANES))
        at += size
    return bounds


def part_tile(part):
    return 384 if part % 384 == 0 else LANES


def tile_of(width):
    for tile in (512, 384, 256):
        if width % tile == 0:
            return tile
    return LANES


def kernels_fit(router_input, router_weight, expert_ids, down_weight, hidden, grad_output):
    groups = lax.axis_size("dp")
    sources = lax.axis_size("expert") * lax.axis_size("tensor")
    slots, width = hidden.shape[1:]
    tokens, model = grad_output.shape
    experts = router_weight.shape[1]
    return (
        groups == 4
        and sources == experts
        and slots % 8 == 0
        and slots // sources == HALF + 1
        and slots <= LANES
        and tokens % 16 == 0
        and width % (groups * LANES) == 0
        and router_input.shape[1] % (lax.axis_size("expert") * LANES) == 0
        and sources * PAD <= LANES
        and 2 * (width * model + 4 * slots * width + 8 * slots * model) < 48 * 1000 * 1000
    )


def per_device(*arrays):
    return by_kernels(*arrays) if kernels_fit(*arrays) else by_collectives(*arrays)


def by_collectives(router_input, router_weight, expert_ids, down_weight, hidden, grad_output):
    token_rows = grad_output.shape[0]
    model_width = grad_output.shape[1]
    expert_count = router_weight.shape[1]
    choose_count = expert_ids.shape[1]
    expert_ranks = lax.axis_size("expert")
    tensor_ranks = lax.axis_size("tensor")
    sources = expert_ranks * tensor_ranks
    spread = sources // expert_count
    capacity = hidden.shape[1] // sources
    full_input = lax.all_to_all(router_input, "tensor", split_axis=0, concat_axis=1, tiled=True)
    logits = jnp.dot(full_input, router_weight, preferred_element_type=jnp.float32)
    labels = jnp.arange(expert_count, dtype=jnp.int32)
    onehot_int = (expert_ids[:, :, None] == labels).astype(jnp.int32)
    onehot = onehot_int.astype(jnp.float32)
    picked = jnp.sum(onehot * logits[:, None, :], axis=2)
    first_gate = jax.nn.sigmoid(picked[:, 0] - picked[:, 1])
    second_gate = jax.nn.sigmoid(picked[:, 1] - picked[:, 0])
    gate_values = jnp.stack([first_gate, second_gate], axis=1)
    gate_low = gate_values.astype(jnp.bfloat16)
    flat_hits = onehot_int.reshape(token_rows * choose_count, expert_count)
    before = jnp.cumsum(flat_hits, axis=0) - flat_hits
    slot_pos = jnp.sum(before * flat_hits, axis=1).reshape(token_rows, choose_count)
    slot_ids = jnp.arange(capacity, dtype=jnp.int32)
    dispatch_table = onehot[:, :, :, None] * (slot_pos[:, :, None, None] == slot_ids).astype(
        jnp.float32
    )
    slot_table = jnp.sum(dispatch_table, axis=1).astype(jnp.bfloat16)
    packed_grad = jnp.einsum(
        "rec,rd->ecd", slot_table, grad_output, preferred_element_type=jnp.float32
    ).astype(jnp.bfloat16)
    packed_gate = jnp.einsum("rkec,rk->ec", dispatch_table, gate_low.astype(jnp.float32)).astype(
        jnp.bfloat16
    )
    send_grad = jnp.repeat(packed_grad, spread, axis=0)
    send_gate = jnp.repeat(packed_gate, spread, axis=0)
    recv_grad, recv_gate = (
        lax.all_to_all(send_grad, ("expert", "tensor"), split_axis=0, concat_axis=0, tiled=True),
        lax.all_to_all(send_gate, ("expert", "tensor"), split_axis=0, concat_axis=0, tiled=True),
    )
    recv_grad = recv_grad.reshape(sources * capacity, model_width)
    recv_gate = recv_gate.reshape(sources * capacity).astype(jnp.float32)
    hidden_rows = hidden[0]
    gated_grad = (recv_gate[:, None] * recv_grad.astype(jnp.float32)).astype(jnp.bfloat16)
    expert_image = lax.dot_general(
        recv_grad, down_weight, (((1,), (1,)), ((), ())), preferred_element_type=jnp.float32
    )
    hidden_part = (recv_gate[:, None] * expert_image).astype(jnp.bfloat16)
    gate_partial = jnp.sum(hidden_rows.astype(jnp.float32) * expert_image, axis=1).reshape(
        sources, capacity
    )
    returned = lax.all_to_all(
        gate_partial, ("expert", "tensor"), split_axis=0, concat_axis=0, tiled=True
    )
    expert_sums = jnp.sum(returned.reshape(expert_count, spread, capacity), axis=1)
    gate_grad = jnp.einsum("rkec,ec->rk", dispatch_table, expert_sums)
    mixed_term = jnp.sum(gate_values * gate_grad, axis=1, keepdims=True)
    logit_part = gate_values * (gate_grad - mixed_term)
    logit_grad = jnp.sum(onehot * logit_part[:, :, None], axis=1)
    input_grad = jnp.dot(
        logit_grad, router_weight.astype(jnp.float32).T, precision=lax.Precision.HIGHEST
    ).astype(jnp.bfloat16)
    router_local = jnp.dot(
        full_input.astype(jnp.float32).T, logit_grad, precision=lax.Precision.HIGHEST
    )
    router_grad = lax.psum(router_local, ("dp", "expert", "tensor"))
    hidden_all = lax.all_to_all(hidden_rows, "dp", split_axis=1, concat_axis=0, tiled=True)
    gated_all = lax.all_gather(gated_grad, "dp", axis=0, tiled=True)
    weight_sum = lax.dot_general(
        hidden_all, gated_all, (((0,), (0,)), ((), ())), preferred_element_type=jnp.float32
    ).astype(jnp.bfloat16)
    return (weight_sum, hidden_part[None], router_grad, input_grad)


def solution(mesh):
    return jax.shard_map(
        per_device,
        mesh=mesh,
        in_specs=(
            P(("dp", "expert"), "tensor"),
            P(),
            P(("dp", "expert", "tensor"), None),
            P(("expert", "tensor"), None),
            P("dp", None, ("expert", "tensor")),
            P(("dp", "expert", "tensor"), None),
        ),
        out_specs=(
            P(("expert", "tensor", "dp"), None),
            P("dp", None, ("expert", "tensor")),
            P(),
            P(("dp", "expert", "tensor"), None),
        ),
        check_vma=False,
    )
```

```python
import functools

import jax
import jax.numpy as jnp
from jax import lax
from jax.experimental import pallas as pl
from jax.experimental.pallas import tpu as pltpu
from jax.sharding import PartitionSpec as P


PAD = 16
LANES = 128
HALF = 8
VMEM_LIMIT = 50 * 1000 * 1000
WEIGHT_LIMIT = 24 * 1000 * 1000
OUT = pltpu.VMEM
PAUSE = 6
LAST_TILES = 4
NEAR_FIFTHS = 3
EXACT = lax.Precision.HIGHEST
CONTRACT_LAST = (((1,), (1,)), ((), ()))
CONTRACT_FIRST = (((0,), (0,)), ((), ()))


def iota(shape, axis):
    return lax.broadcasted_iota(jnp.int32, shape, axis)


def exchange_kernel(
    groups, expert_ranks, tensor_ranks, capacity, tile,
    ids_hbm, router_weight_hbm, grad_hbm, router_input_ref, down_ref, hidden_ref,
    near_ref, hidden_near, gated_near, hidden_far, gated_far, hidden_out, input_grad_ref,
    router_grad_ref, ids_ref, router_weight_ref, grad_ref, own_input, weights, hidden_rows,
    send_low, recv_low, send_top, recv_top, send_back, recv_back,
    send_info, recv_info, column_input, slot_weight, slot_sign, logit_rows, group_sums,
    send_logit, recv_logit, packed, pulled,
    load_sem, weight_sem, hidden_sem, own_sem,
    logit_send, logit_recv, low_send, low_recv, top_send, top_recv,
    hidden_send, hidden_recv, gated_send, gated_recv, back_send, back_recv,
    info_send, info_recv, column_send, column_recv, sum_send, sum_recv, whole_send, whole_recv,
):
    f32, bf16 = jnp.float32, jnp.bfloat16
    group = lax.axis_index("dp")
    expert = lax.axis_index("expert")
    tensor = lax.axis_index("tensor")
    sources = expert_ranks * tensor_ranks
    source = expert * tensor_ranks + tensor
    slots, width = hidden_ref.shape
    part = width // groups
    experts = router_weight_ref.shape[0]
    tokens = grad_ref.shape[0]
    span = router_input_ref.shape[1]
    feats = span // expert_ranks
    rows = sources * PAD
    tiles = width // tile

    def remote(src, dst, send, recv, device):
        return pltpu.make_async_remote_copy(
            src_ref=src, dst_ref=dst, send_sem=send, recv_sem=recv,
            device_id=device, device_id_type=pl.DeviceIdType.MESH,
        )

    def drain(ref, sem):
        pltpu.make_async_copy(ref, ref, sem).wait()

    cuts = chunk_bounds(tiles)
    weight_copies = [
        pltpu.make_async_copy(
            down_ref.at[pl.ds(begin * tile, (end - begin) * tile)],
            weights.at[pl.ds(begin * tile, (end - begin) * tile)], weight_sem.at[c],
        )
        for c, (begin, end) in enumerate(cuts)
    ]

    ers = [(expert + e) % expert_ranks for e in range(expert_ranks)]
    trs = [(tensor + t) % tensor_ranks for t in range(tensor_ranks)]
    peers = [
        (ers[e] * tensor_ranks + trs[t], {"dp": group, "expert": ers[e], "tensor": trs[t]})
        for e in sorted(range(expert_ranks), key=lambda e: abs(2 * e - expert_ranks))
        for t in range(tensor_ranks) if e or t
    ]
    core = group % 2
    half = group // 2
    beside = half * 2 + (1 - core)
    across = (1 - half) * 2 + core
    diagonal = (1 - half) * 2 + (1 - core)
    mates = [
        {"dp": to, "expert": expert, "tensor": tensor} for to in (across, diagonal, beside)
    ]

    loads = [
        pltpu.make_async_copy(ids_hbm, ids_ref, load_sem.at[0]),
        pltpu.make_async_copy(grad_hbm, grad_ref, load_sem.at[1]),
        pltpu.make_async_copy(router_weight_hbm, router_weight_ref, load_sem.at[2]),
        pltpu.make_async_copy(router_input_ref, own_input, load_sem.at[3]),
        pltpu.make_async_copy(
            router_input_ref.at[:, pl.ds(pl.multiple_of(expert * feats, LANES), feats)],
            column_input.at[expert], load_sem.at[4],
        ),
    ]
    for copy in loads:
        copy.start()

    hidden_load = pltpu.make_async_copy(hidden_ref, hidden_rows, hidden_sem)
    hidden_load.start()

    for copy in weight_copies:
        copy.start(priority=1)
    own_hidden = pltpu.make_async_copy(
        hidden_ref.at[:, pl.ds(pl.multiple_of(group * part, LANES), part)],
        hidden_near.at[0, pl.ds(0, slots)], own_sem,
    )
    own_hidden.start()

    barrier = pltpu.get_barrier_semaphore()
    for where in [place for _, place in peers] + mates:
        pl.semaphore_signal(
            barrier, inc=1, device_id=where, device_id_type=pl.DeviceIdType.MESH
        )

    send_info[...] = jnp.zeros_like(send_info)
    tail = hidden_near.shape[1] - slots
    for buffer in (hidden_near, hidden_far, gated_near, gated_far):
        buffer[:, slots:, :] = jnp.zeros((2, tail, buffer.shape[2]), bf16)
    for copy in loads[:4]:
        copy.wait()
    labels = iota((experts, tokens), 0)
    pick_first = (ids_ref[0:1, :] == labels).astype(f32)
    pick_second = (ids_ref[1:2, :] == labels).astype(f32)
    pick_both = pick_first + pick_second
    earlier = (iota((tokens, tokens), 1) < iota((tokens, tokens), 0)).astype(f32)
    before = lax.dot_general(pick_both, earlier, CONTRACT_LAST, preferred_element_type=f32)
    spread_rows = ((iota((rows, experts), 0) >> 4) == iota((rows, experts), 1)).astype(f32)
    hit = jnp.dot(spread_rows, pick_both, preferred_element_type=f32)
    rank = jnp.dot(spread_rows, before, preferred_element_type=f32)
    slot = (iota((rows, tokens), 0) & (PAD - 1)).astype(f32)
    table = jnp.where((hit > 0.5) & (jnp.abs(rank - slot) < 0.5), 1.0, 0.0).astype(f32)
    low_table = table.reshape(sources, PAD, tokens)[:, :HALF].reshape(sources * HALF, tokens)
    top_table = jnp.where((pick_both > 0.5) & (jnp.abs(before - HALF) < 0.5), 1.0, 0.0)
    wide = send_low.shape[3]
    for h in range(2):
        send_low[h] = (
            jnp.dot(
                low_table.astype(bf16), grad_ref[:, h * wide : (h + 1) * wide],
                preferred_element_type=f32,
            )
            .astype(bf16)
            .reshape(send_low.shape[1:])
        )
    send_top[...] = jnp.dot(
        top_table.astype(bf16), grad_ref[...], preferred_element_type=f32
    ).reshape(send_top.shape)

    own_weight = router_weight_ref[:, pl.ds(pl.multiple_of(tensor * span, LANES), span)]

    def part_logits(t):
        return lax.dot_general(
            own_weight, own_input[pl.ds(pl.multiple_of(trs[t] * tokens, tokens), tokens)],
            CONTRACT_LAST, preferred_element_type=f32,
        )

    for t in range(1, tensor_ranks):
        send_logit[t] = part_logits(t)
    send_logit[0] = part_logits(0)

    pl.semaphore_wait(barrier, len(peers) + len(mates))

    for t in range(1, tensor_ranks):
        remote(
            send_logit.at[t], recv_logit.at[t], logit_send, logit_recv, {"tensor": trs[t]}
        ).start()
    for to, where in peers:
        remote(
            send_low.at[:, to], recv_low.at[:, source], low_send, low_recv, where
        ).start()
    for to, where in peers:
        remote(send_top.at[to], recv_top.at[source], top_send, top_recv, where).start()

    hidden_to = (
        (beside, hidden_near.at[1, pl.ds(0, slots)], 0),
        (across, hidden_far.at[0, pl.ds(0, slots)], 1),
        (diagonal, hidden_far.at[1, pl.ds(0, slots)], 2),
    )
    hidden_copies = [
        remote(
            hidden_rows.at[:, pl.ds(pl.multiple_of(to * part, LANES), part)], landing,
            hidden_send.at[k], hidden_recv.at[k], {"dp": to},
        )
        for to, landing, k in hidden_to
    ]
    hidden_load.wait()
    for copy in hidden_copies:
        copy.start()

    recv_top[pl.ds(source, 1)] = send_top[pl.ds(source, 1)]
    for h in range(2):
        recv_low[h, pl.ds(source, 1)] = send_low[h, pl.ds(source, 1)]

    height = packed.shape[0]
    column = iota((height, sources * HALF), 1)
    pick_low = (
        iota((height, sources * HALF), 0) == capacity * (column >> 3) + (column & (HALF - 1))
    ).astype(bf16)
    slot_row = iota((height, sources), 0)
    slot_base = capacity * iota((height, sources), 1)
    pick_top = (slot_row == slot_base + HALF).astype(bf16)
    pick_source = ((slot_row >= slot_base) & (slot_row < slot_base + capacity)).astype(f32)
    slot_at = iota((height, LANES), 0) - capacity * jnp.sum(
        pick_source * iota((height, sources), 1).astype(f32), axis=1, keepdims=True
    ).astype(jnp.int32)
    slot_lane = (slot_at == iota((height, LANES), 1)) & (iota((height, LANES), 0) < slots)

    def pull(c):
        begin, end = cuts[c]
        weight_copies[c].wait()
        at = slice(begin * tile, end * tile)
        term = jnp.dot(hidden_rows[:, at], weights[at, :], preferred_element_type=f32)
        pulled[...] = pulled[...] + term if c else term

    early = 1
    for c in range(early):
        pull(c)

    drain(recv_logit.at[pl.ds(0, tensor_ranks - 1)], logit_recv)
    logits = send_logit[0]
    for t in range(1, tensor_ranks):
        logits = logits + recv_logit[t]
    chosen = jnp.sum(pick_first * logits, axis=0, keepdims=True)
    rival = jnp.sum(pick_second * logits, axis=0, keepdims=True)
    first_gate = jax.nn.sigmoid(chosen - rival)
    second_gate = jax.nn.sigmoid(rival - chosen)
    numbered = before + PAD * labels.astype(f32)
    send_info[0:1, :tokens] = jnp.sum(pick_first * numbered, axis=0, keepdims=True)
    send_info[1:2, :tokens] = jnp.sum(pick_second * numbered, axis=0, keepdims=True)
    send_info[2:3, :tokens] = first_gate * second_gate
    send_info[3:4, :tokens] = first_gate.astype(bf16).astype(f32)
    send_info[4:5, :tokens] = second_gate.astype(bf16).astype(f32)
    for _, where in peers:
        remote(send_info, recv_info.at[source], info_send, info_recv, where).start()
    recv_info[pl.ds(source, 1)] = send_info[...][None]

    for c in range(early, len(cuts)):
        pull(c)

    drain(recv_info.at[pl.ds(0, sources - 1)], info_recv)
    drain(recv_low.at[:, pl.ds(0, sources - 1)], low_recv)
    drain(recv_top.at[pl.ds(0, sources - 1)], top_recv)
    model = packed.shape[1]
    for h in range(2):
        at = slice(h * wide, (h + 1) * wide)
        packed[:, at] = (
            jnp.dot(
                pick_low, recv_low[h].reshape(sources * HALF, wide), preferred_element_type=f32
            )
            + jnp.dot(
                pick_top, recv_top[:, :, at].reshape(sources, wide).astype(bf16),
                preferred_element_type=f32,
            )
        ).astype(bf16)
    partial = jnp.sum(packed[:slots].astype(f32) * pulled[...], axis=1, keepdims=True)
    own_lane = (iota((slots, LANES), 1) - PAD * source) == slot_at[:slots]
    send_back[...] = lax.dot_general(
        pick_source[:slots], jnp.where(own_lane, partial, 0.0), CONTRACT_FIRST,
        precision=EXACT, preferred_element_type=f32,
    )
    for _, where in peers:
        remote(send_back, recv_back.at[source], back_send, back_recv, where).start()
    for e in range(1, expert_ranks):
        remote(
            own_input.at[:, pl.ds(pl.multiple_of(ers[e] * feats, LANES), feats)],
            column_input.at[expert], column_send, column_recv, {"expert": ers[e]},
        ).start()
    recv_back[pl.ds(source, 1)] = send_back[...][None]

    known = recv_info[...].reshape(sources * HALF, LANES)
    known = jnp.concatenate([known, jnp.zeros((LANES - sources * HALF, LANES), f32)], axis=0).T
    slot_lanes = iota((tokens, LANES), 1).astype(f32)
    label_lanes = PAD * iota((tokens, experts), 1).astype(f32)
    gate_lanes = jnp.zeros((height, LANES), f32)
    for x in range(sources):
        one, two, share, one_gate, two_gate = (
            known[:tokens, x * HALF + k : x * HALF + k + 1] for k in range(5)
        )
        slot_weight[x] = jnp.where(
            slot_lanes == one, share, jnp.where(slot_lanes == two, -share, 0.0)
        )
        slot_sign[x] = jnp.where(
            (one >= label_lanes) & (one < label_lanes + PAD), 1.0, 0.0
        ) - jnp.where((two >= label_lanes) & (two < label_lanes + PAD), 1.0, 0.0)
        gate_row = jnp.sum(
            jnp.where(
                slot_lanes == one, one_gate, jnp.where(slot_lanes == two, two_gate, 0.0)
            ),
            axis=0, keepdims=True,
        )
        gate_lanes = gate_lanes + pick_source[:, x : x + 1] * gate_row
    gate_column = jnp.sum(
        jnp.where(own_lane, gate_lanes[:slots], 0.0), axis=1, keepdims=True
    )
    gated_near[0, :slots] = (gate_column * packed[:slots].astype(f32)).astype(bf16)

    fold = model * 3 // 8 // LANES * LANES
    spans = (pl.ds(0, fold), pl.ds(fold, model - fold))

    def gated_part(buffer, k, h):
        return buffer.at[k, pl.ds(0, slots), spans[h]]

    to_across, to_beside, relays = [], [], []
    for h in range(2):
        mine = gated_part(gated_near, 0, h)
        from_beside = gated_part(gated_near, 1, h)
        from_across = gated_part(gated_far, 0, h)
        from_diagonal = gated_part(gated_far, 1, h)
        to_across.append(
            remote(mine, from_across, gated_send.at[0, h], gated_recv.at[0, h], {"dp": across})
        )
        to_beside.append(
            remote(mine, from_beside, gated_send.at[1, h], gated_recv.at[1, h], {"dp": beside})
        )
        relays.append(
            remote(
                from_across, from_diagonal, gated_send.at[2, h], gated_recv.at[2, h],
                {"dp": beside},
            )
        )
    to_across[0].start()
    for copy in to_beside:
        copy.start()

    def image_tile(i):
        at = slice(i * tile, (i + 1) * tile)
        image = lax.dot_general(
            weights[at, :], packed[...], CONTRACT_LAST, preferred_element_type=f32
        ).T[:slots]
        hidden_out[:, at] = (gate_column * image).astype(bf16)

    pause = tiles * PAUSE // 15
    for i in range(pause):
        image_tile(i)

    drain(recv_back.at[pl.ds(0, sources - 1)], back_recv)
    returned = recv_back[0]
    for e in range(1, experts):
        returned = returned + recv_back[e]
    for x in range(sources):
        logit_rows[x] = slot_sign[x] * jnp.sum(
            slot_weight[x] * returned[x : x + 1], axis=1, keepdims=True
        )
    terms = split_terms(logit_rows[...].reshape(sources * tokens, experts))
    loads[4].wait()
    drain(column_input.at[pl.ds(0, expert_ranks - 1)], column_recv)
    sums = lax.dot_general(
        terms, column_input[...].reshape(sources * tokens, feats), CONTRACT_FIRST,
        preferred_element_type=f32,
    )
    group_sums[pl.ds(group, 1)] = (
        sums[:experts] + sums[experts : 2 * experts] + sums[2 * experts :]
    )[None]
    for where in mates:
        remote(
            group_sums.at[group], group_sums.at[group], sum_send, sum_recv, where
        ).start()
    to_across[1].start()
    input_grad_ref[...] = jnp.dot(
        logit_rows[pl.ds(source, 1)].reshape(tokens, experts),
        router_weight_ref[...].astype(f32), precision=EXACT,
        preferred_element_type=f32,
    ).astype(bf16)

    later = max(pause, tiles - LAST_TILES)
    for i in range(pause, later):
        image_tile(i)

    to_across[0].wait_recv()
    relays[0].start()
    drain(group_sums.at[pl.ds(0, groups - 1)], sum_recv)
    total = group_sums[0]
    for d in range(1, groups):
        total = total + group_sums[d]
    router_grad_ref[pl.ds(source, 1)] = total[None]
    for _, where in peers:
        remote(
            router_grad_ref.at[source], router_grad_ref.at[source], whole_send, whole_recv, where
        ).start()
    for i in range(later, tiles):
        image_tile(i)


    step = part_tile(part)

    to_across[1].wait_recv()
    relays[1].start()
    own_hidden.wait()
    hidden_copies[0].wait_recv()
    for copy in to_beside:
        copy.wait_recv()
    for i in range(near_ref.shape[0] // step):
        at = slice(i * step, (i + 1) * step)
        near_ref[at, :] = pair_product(hidden_near, gated_near, at).astype(bf16)

    for copy in hidden_copies[1:]:
        copy.wait_recv()
    for copy in relays:
        copy.wait_recv()
    for copy in (*hidden_copies, *to_across, *to_beside, *relays):
        copy.wait_send()
    drain(send_low.at[:, pl.ds(0, sources - 1)], low_send)
    drain(send_top.at[pl.ds(0, sources - 1)], top_send)
    drain(recv_logit.at[pl.ds(0, tensor_ranks - 1)], logit_send)
    drain(recv_back.at[pl.ds(0, sources - 1)], back_send)
    drain(recv_info.at[pl.ds(0, sources - 1)], info_send)
    drain(column_input.at[pl.ds(0, expert_ranks - 1)], column_send)
    drain(group_sums.at[pl.ds(0, groups - 1)], sum_send)
    drain(router_grad_ref.at[pl.ds(0, sources - 1)], whole_recv)
    drain(router_grad_ref.at[pl.ds(0, sources - 1)], whole_send)


def split_terms(value):
    parts = []
    for _ in range(3):
        part = value.astype(jnp.bfloat16).astype(jnp.float32)
        parts.append(part)
        value = value - part
    return jnp.concatenate(parts, axis=1).astype(jnp.bfloat16)


def chunk_bounds(tiles):
    bounds, at = [], 0
    while at < tiles:
        size = 3 if tiles - at > 3 else max(1, (tiles - at) // 2 + (tiles - at) % 2)
        bounds.append((at, at + size))
        at += size
    return bounds


def pair_product(hidden_ref, gated_ref, at):
    depth = hidden_ref.shape[0] * hidden_ref.shape[1]
    return lax.dot_general(
        hidden_ref[:, :, at].reshape(depth, at.stop - at.start),
        gated_ref[...].reshape(depth, gated_ref.shape[2]),
        CONTRACT_FIRST, preferred_element_type=jnp.float32,
    )


def weight_kernel(
    tensor_ranks, near_ref, hidden_near, gated_near, hidden_far, gated_far, hidden_ref, input_ref, router_ref,
    weight_out, hidden_out, input_out, router_out, weight_rows, router_rows, store_sem,
):
    bounds = row_bounds(weight_rows.shape[0])
    ready = near_ref.shape[0]
    cuts = len(bounds)
    stores = [
        pltpu.make_async_copy(hidden_ref, hidden_out, store_sem.at[cuts]),
        pltpu.make_async_copy(input_ref, input_out, store_sem.at[cuts + 1]),
    ]
    for store in stores:
        store.start()
    for c, (begin, end) in enumerate(bounds):
        at = slice(begin, end)
        far = pair_product(hidden_far, gated_far, at)
        if end <= ready:
            near = near_ref[at, :].astype(jnp.float32)
        else:
            near = pair_product(hidden_near, gated_near, at)
        weight_rows[at, :] = (far + near).astype(weight_rows.dtype)
        rows = pl.ds(begin, end - begin)
        stores.append(
            pltpu.make_async_copy(weight_rows.at[rows], weight_out.at[rows], store_sem.at[c])
        )
        stores[-1].start()
    sources, _, feats = router_ref.shape
    for x in range(sources):
        e, t = x // tensor_ranks, x % tensor_ranks
        column = (t * (sources // tensor_ranks) + e) * feats
        router_rows[:, column : column + feats] = router_ref[x]
    stores.append(pltpu.make_async_copy(router_rows, router_out, store_sem.at[cuts + 2]))
    stores[-1].start()
    for store in stores:
        store.wait()


def by_kernels(router_input, router_weight, expert_ids, down_weight, hidden, grad_output):
    f32, bf16 = jnp.float32, jnp.bfloat16
    tokens, model = grad_output.shape
    experts = router_weight.shape[1]
    groups = lax.axis_size("dp")
    expert_ranks = lax.axis_size("expert")
    tensor_ranks = lax.axis_size("tensor")
    sources = expert_ranks * tensor_ranks
    slots, width = hidden.shape[1:]
    height = -(-slots // LANES) * LANES
    tile = tile_of(width)
    span = router_input.shape[1]
    part = width // groups
    vmem = pl.BlockSpec(memory_space=pltpu.VMEM)
    hbm = pl.BlockSpec(memory_space=pl.ANY)
    dma = pltpu.SemaphoreType.DMA
    feats = span // expert_ranks
    near, *pairs, hidden_grad, input_grad, router_parts = pl.pallas_call(
        functools.partial(
            exchange_kernel, groups, expert_ranks, tensor_ranks, slots // sources, tile
        ),
        out_shape=(
            OUT((near_rows(part), model), bf16),
            OUT((2, height, part), bf16),
            OUT((2, height, model), bf16),
            OUT((2, height, part), bf16),
            OUT((2, height, model), bf16),
            OUT((slots, width), bf16),
            OUT((tokens, model), bf16),
            OUT((sources, experts, feats), f32),
        ),
        in_specs=[hbm] * 6,
        out_specs=(vmem,) * 8,
        scratch_shapes=[
            pltpu.VMEM((2, tokens), jnp.int32),
            pltpu.VMEM((experts, model), bf16),
            pltpu.VMEM((tokens, model), bf16),
            pltpu.VMEM((tensor_ranks * tokens, span), bf16),
            pltpu.VMEM((width, model), bf16),
            pltpu.VMEM((slots, width), bf16),
            pltpu.VMEM((2, sources, HALF, model // 2), bf16),
            pltpu.VMEM((2, sources, HALF, model // 2), bf16),
            pltpu.VMEM((sources, 1, model), f32),
            pltpu.VMEM((sources, 1, model), f32),
            pltpu.VMEM((sources, LANES), f32),
            pltpu.VMEM((experts, sources, LANES), f32),
            pltpu.VMEM((HALF, LANES), f32),
            pltpu.VMEM((sources, HALF, LANES), f32),
            pltpu.VMEM((expert_ranks, tensor_ranks * tokens, feats), bf16),
            pltpu.VMEM((sources, tokens, LANES), f32),
            pltpu.VMEM((sources, tokens, experts), f32),
            pltpu.VMEM((sources, tokens, experts), f32),
            pltpu.VMEM((groups, experts, feats), f32),
            pltpu.VMEM((tensor_ranks, experts, tokens), f32),
            pltpu.VMEM((tensor_ranks, experts, tokens), f32),
            pltpu.VMEM((height, model), bf16),
            pltpu.VMEM((slots, model), f32),
            dma((5,)), dma((len(chunk_bounds(width // tile)),)), dma, dma,
            dma, dma, dma, dma, dma, dma,
            dma((3,)), dma((3,)), dma((3, 2)), dma((3, 2)), dma, dma,
            dma, dma, dma, dma, dma, dma, dma, dma,
        ],
        compiler_params=pltpu.CompilerParams(
            collective_id=0, has_side_effects=True, vmem_limit_bytes=VMEM_LIMIT
        ),
        name="exchange",
    )(expert_ids.T, router_weight.T, grad_output, router_input, down_weight, hidden[0])
    weight_grad, hidden_grad, input_grad, router_grad = pl.pallas_call(
        functools.partial(weight_kernel, tensor_ranks),
        out_shape=(
            jax.ShapeDtypeStruct((part, model), bf16),
            jax.ShapeDtypeStruct((slots, width), bf16),
            jax.ShapeDtypeStruct((tokens, model), bf16),
            jax.ShapeDtypeStruct((experts, model), f32),
        ),
        in_specs=[vmem] * 8,
        out_specs=(hbm,) * 4,
        scratch_shapes=[
            pltpu.VMEM((part, model), bf16),
            pltpu.VMEM((experts, model), f32),
            dma((len(row_bounds(part)) + 3,)),
        ],
        compiler_params=pltpu.CompilerParams(vmem_limit_bytes=WEIGHT_LIMIT),
        name="weight_grad",
    )(near, *pairs, hidden_grad, input_grad, router_parts)
    return weight_grad, hidden_grad[None], router_grad.T, input_grad


def near_rows(part):
    step = part_tile(part)
    return max(1, part // step * NEAR_FIFTHS // 5) * step


def row_bounds(part):
    units, ready, bounds, at = part // LANES, near_rows(part) // LANES, [], 0
    while at < units:
        stop = ready if at < ready else units
        size = min(stop - at, 2 if at == 0 or at >= ready else 3)
        bounds.append((at * LANES, (at + size) * LANES))
        at += size
    return bounds


def part_tile(part):
    return 384 if part % 384 == 0 else LANES


def tile_of(width):
    for tile in (512, 384, 256):
        if width % tile == 0:
            return tile
    return LANES


def kernels_fit(router_input, router_weight, expert_ids, down_weight, hidden, grad_output):
    groups = lax.axis_size("dp")
    sources = lax.axis_size("expert") * lax.axis_size("tensor")
    slots, width = hidden.shape[1:]
    tokens, model = grad_output.shape
    experts = router_weight.shape[1]
    return (
        groups == 4
        and sources == experts
        and slots % 8 == 0
        and slots // sources == HALF + 1
        and slots <= LANES
        and tokens % 16 == 0
        and width % (groups * LANES) == 0
        and router_input.shape[1] % (lax.axis_size("expert") * LANES) == 0
        and sources * PAD <= LANES
        and 2 * (width * model + 4 * slots * width + 8 * slots * model) < 48 * 1000 * 1000
    )


def per_device(*arrays):
    return by_kernels(*arrays) if kernels_fit(*arrays) else by_collectives(*arrays)


def by_collectives(router_input, router_weight, expert_ids, down_weight, hidden, grad_output):
    token_rows = grad_output.shape[0]
    model_width = grad_output.shape[1]
    expert_count = router_weight.shape[1]
    choose_count = expert_ids.shape[1]
    expert_ranks = lax.axis_size("expert")
    tensor_ranks = lax.axis_size("tensor")
    sources = expert_ranks * tensor_ranks
    spread = sources // expert_count
    capacity = hidden.shape[1] // sources
    full_input = lax.all_to_all(router_input, "tensor", split_axis=0, concat_axis=1, tiled=True)
    logits = jnp.dot(full_input, router_weight, preferred_element_type=jnp.float32)
    labels = jnp.arange(expert_count, dtype=jnp.int32)
    onehot_int = (expert_ids[:, :, None] == labels).astype(jnp.int32)
    onehot = onehot_int.astype(jnp.float32)
    picked = jnp.sum(onehot * logits[:, None, :], axis=2)
    first_gate = jax.nn.sigmoid(picked[:, 0] - picked[:, 1])
    second_gate = jax.nn.sigmoid(picked[:, 1] - picked[:, 0])
    gate_values = jnp.stack([first_gate, second_gate], axis=1)
    gate_low = gate_values.astype(jnp.bfloat16)
    flat_hits = onehot_int.reshape(token_rows * choose_count, expert_count)
    before = jnp.cumsum(flat_hits, axis=0) - flat_hits
    slot_pos = jnp.sum(before * flat_hits, axis=1).reshape(token_rows, choose_count)
    slot_ids = jnp.arange(capacity, dtype=jnp.int32)
    dispatch_table = onehot[:, :, :, None] * (slot_pos[:, :, None, None] == slot_ids).astype(
        jnp.float32
    )
    slot_table = jnp.sum(dispatch_table, axis=1).astype(jnp.bfloat16)
    packed_grad = jnp.einsum(
        "rec,rd->ecd", slot_table, grad_output, preferred_element_type=jnp.float32
    ).astype(jnp.bfloat16)
    packed_gate = jnp.einsum("rkec,rk->ec", dispatch_table, gate_low.astype(jnp.float32)).astype(
        jnp.bfloat16
    )
    send_grad = jnp.repeat(packed_grad, spread, axis=0)
    send_gate = jnp.repeat(packed_gate, spread, axis=0)
    recv_grad, recv_gate = (
        lax.all_to_all(send_grad, ("expert", "tensor"), split_axis=0, concat_axis=0, tiled=True),
        lax.all_to_all(send_gate, ("expert", "tensor"), split_axis=0, concat_axis=0, tiled=True),
    )
    recv_grad = recv_grad.reshape(sources * capacity, model_width)
    recv_gate = recv_gate.reshape(sources * capacity).astype(jnp.float32)
    hidden_rows = hidden[0]
    gated_grad = (recv_gate[:, None] * recv_grad.astype(jnp.float32)).astype(jnp.bfloat16)
    expert_image = lax.dot_general(
        recv_grad, down_weight, (((1,), (1,)), ((), ())), preferred_element_type=jnp.float32
    )
    hidden_part = (recv_gate[:, None] * expert_image).astype(jnp.bfloat16)
    gate_partial = jnp.sum(hidden_rows.astype(jnp.float32) * expert_image, axis=1).reshape(
        sources, capacity
    )
    returned = lax.all_to_all(
        gate_partial, ("expert", "tensor"), split_axis=0, concat_axis=0, tiled=True
    )
    expert_sums = jnp.sum(returned.reshape(expert_count, spread, capacity), axis=1)
    gate_grad = jnp.einsum("rkec,ec->rk", dispatch_table, expert_sums)
    mixed_term = jnp.sum(gate_values * gate_grad, axis=1, keepdims=True)
    logit_part = gate_values * (gate_grad - mixed_term)
    logit_grad = jnp.sum(onehot * logit_part[:, :, None], axis=1)
    input_grad = jnp.dot(
        logit_grad, router_weight.astype(jnp.float32).T, precision=lax.Precision.HIGHEST
    ).astype(jnp.bfloat16)
    router_local = jnp.dot(
        full_input.astype(jnp.float32).T, logit_grad, precision=lax.Precision.HIGHEST
    )
    router_grad = lax.psum(router_local, ("dp", "expert", "tensor"))
    hidden_all = lax.all_to_all(hidden_rows, "dp", split_axis=1, concat_axis=0, tiled=True)
    gated_all = lax.all_gather(gated_grad, "dp", axis=0, tiled=True)
    weight_sum = lax.dot_general(
        hidden_all, gated_all, (((0,), (0,)), ((), ())), preferred_element_type=jnp.float32
    ).astype(jnp.bfloat16)
    return (weight_sum, hidden_part[None], router_grad, input_grad)


def solution(mesh):
    return jax.shard_map(
        per_device,
        mesh=mesh,
        in_specs=(
            P(("dp", "expert"), "tensor"),
            P(),
            P(("dp", "expert", "tensor"), None),
            P(("expert", "tensor"), None),
            P("dp", None, ("expert", "tensor")),
            P(("dp", "expert", "tensor"), None),
        ),
        out_specs=(
            P(("expert", "tensor", "dp"), None),
            P("dp", None, ("expert", "tensor")),
            P(),
            P(("dp", "expert", "tensor"), None),
        ),
        check_vma=False,
    )
```
